32 devices in a mesh: dp: 16 (over z, x, core), expert: 2 (over y).
Axes of the slice: x: 2, y: 2, z: 4, core: 2. Of those that a mesh axis runs over, the one named last changes fastest.
Arguments:
- x_rows: bfloat16 [16384, 1024], P(('dp', 'expert')), may hold values from -6 to 6
- dy_rows: bfloat16 [16384, 2048], P(('dp', 'expert')), may hold values from -0.0625 to 0.0625
- seg_blocks: int32 [32, 2], replicated, may hold values from 0 to 2, as said below
Outputs:
- expert_grad: float32 [2, 1024, 2048], P(None, 'dp', 'expert')
The draws below stay inside these ranges and needn't reach their ends.
Inputs may be any that keep to these rules, and one draw needn't show every extreme that they name: `seg_blocks`: on every device the entries sum to at most 4; one expert has exactly 2 blocks on every device.
All inputs are finite; a program needn't handle non-finite values.
Results may differ from the reference program's by a relative error of at most 0.0003.
Values may be sent and summed in bfloat16 or wider, within the bound.
A program may use at most 128 MiB of HBM per device.

```python
import jax
import jax.numpy as jnp
from jax import lax

H = 1024
F = 2048
BLOCK = 128
CAP = 2
BLOCKS_DEV = 4
EXPERTS = 2
SHARDS = 32
ROWS = 16384


def draw_seg_blocks(key, part):
    hot = jax.random.randint(jax.random.fold_in(key, 7), (), 0, EXPERTS)
    room = min(BLOCKS_DEV, CAP * EXPERTS) - CAP
    experts_row = jnp.arange(EXPERTS, dtype=jnp.int32)

    def single(device):
        sub = jax.random.fold_in(jax.random.fold_in(key, 11), device)
        order = jax.random.permutation(sub, CAP * EXPERTS)
        slot_expert = (order // CAP).astype(jnp.int32)
        others = (slot_expert != hot).astype(jnp.int32)
        rank = jnp.cumsum(others) - 1
        taken = jax.random.randint(jax.random.fold_in(sub, 3), (), room // 2, room + 1)
        chosen = others * (rank < taken).astype(jnp.int32)
        counts = jnp.sum(chosen[:, None] * (slot_expert[:, None] == experts_row[None, :]).astype(jnp.int32), axis=0)
        return (counts + CAP * (experts_row == hot).astype(jnp.int32)).astype(jnp.int32)
    return jax.vmap(single)(jnp.arange(SHARDS, dtype=jnp.int32))


def strengthened(values, own_key, source, target, shards_of, factor):
    owner, partner = [(jnp.arange(values.shape[dim]) // (values.shape[dim] // shards_of)).reshape([-1 if axis == dim else 1 for axis in range(values.ndim)]) for dim in (source, target)]
    chosen = jax.random.permutation(own_key, shards_of)[partner]
    strong = (owner == chosen) | (owner == (partner + shards_of // 2) % shards_of)
    return jnp.where(strong, factor * values, values)


def steps_of(key, extent, shards, least, largest):
    level, own = 1.0, jax.random.fold_in(key, 6)
    for position, blocks in shards:
        draws = jnp.exp(jax.random.uniform(jax.random.fold_in(own, position), (blocks,), jnp.float32, least / len(shards), largest / len(shards)))
        level = level * jnp.repeat(draws, extent[position] // blocks).reshape([-1 if axis == position else 1 for axis in range(len(extent))])
    return level


def scatter_about(own_key, shape, width, limit, cuts=(), kind=jnp.bfloat16):
    values = width * jax.random.normal(own_key, shape, jnp.float32)
    if cuts:
        values = values * steps_of(own_key, shape, cuts, -0.22, 0.18)
    return jnp.clip(values, -limit, limit).astype(kind)


def gaussian_with(own_key, extent, deviation, bound, cuts, heavy, kind=jnp.bfloat16):
    array = deviation * jax.random.normal(own_key, extent, jnp.float32)
    if cuts:
        array = array * steps_of(own_key, extent, cuts, -0.22, 0.18)
    return jnp.clip(strengthened(array, jax.random.fold_in(own_key, 3), *heavy), -bound, bound).astype(kind)


def setup_inputs(seed: int = 0) -> dict:
    keys = jax.random.split(jax.random.key(seed), 4)
    return {
        "x_rows": gaussian_with(keys[0], (ROWS, H), 1.0, 6.0, ((0, 32),), (0, 1, 32, 2.75)),
        "dy_rows": scatter_about(keys[1], (ROWS, F), (SHARDS * CAP * BLOCK) ** -0.5, 0.0625, ((0, 32),)),
        "seg_blocks": draw_seg_blocks(jax.random.fold_in(keys[3], 71), 0),
    }


def pack(xdev, dydev, counts):
    nblk = xdev.shape[0] // BLOCK
    counts = counts.astype(jnp.int32)
    starts = (jnp.cumsum(counts) - counts).astype(jnp.int32)
    slots = jnp.arange(CAP, dtype=jnp.int32)
    live = slots[None, :] < counts[:, None]
    index = jnp.where(live, starts[:, None] + slots[None, :], 0).reshape(-1).astype(jnp.int32)
    keep = live.reshape(-1)[:, None, None]
    xblk = jnp.where(keep, xdev.reshape(nblk, BLOCK, -1)[index], jnp.zeros((), xdev.dtype))
    dyblk = jnp.where(keep, dydev.reshape(nblk, BLOCK, -1)[index], jnp.zeros((), dydev.dtype))
    return xblk, dyblk


def reference(x_rows, dy_rows, seg_blocks):
    xs = x_rows.reshape(SHARDS, -1, H)
    dys = dy_rows.reshape(SHARDS, -1, F)

    def step(total, item):
        xdev, dydev, counts = item
        xblk, dyblk = pack(xdev, dydev, counts)
        xblk = xblk.reshape(EXPERTS, CAP * BLOCK, H).astype(jnp.float32)
        dyblk = dyblk.reshape(EXPERTS, CAP * BLOCK, F).astype(jnp.float32)
        return total + jnp.einsum("erh,erf->ehf", xblk, dyblk), None

    init = jnp.zeros((EXPERTS, H, F), jnp.float32)
    total, _ = lax.scan(step, init, (xs, dys, seg_blocks))
    return total
```

```python
import functools
import math

import jax
import jax.numpy as jnp
from jax import lax
from jax.experimental import pallas as pl
from jax.experimental.pallas import tpu as pltpu
from jax.sharding import PartitionSpec as P

BLOCK = 128
MESH = pl.DeviceIdType.MESH
TOP = 32767.0
PARTS = 4
UNROLL = 2
LINK = 46.6e3
LATENCY = 2.5


def bits_of(size):
    count = size.bit_length() - 1
    assert size == 1 << count
    return count


def plan(n_dp, n_exp, streams, size):
    dp = [("dp", b) for b in range(1, bits_of(n_dp))]
    ex = [("expert", b) for b in range(bits_of(n_exp))]
    first, rest = dp[:1], dp[1:]
    ways = (first + ex + rest, ex + rest[:1] + first + rest[1:], rest[:1] + first + ex + rest[1:])
    orders = [ways[s % len(ways)] for s in range(streams)]
    steps = len(orders[0])
    free, ready, done, turns, clock = {}, [], [0] * streams, [], 0.0

    def sent(s, k, now):
        way = orders[s][k]
        begin = max(now, free.get(way, 0.0))
        free[way] = begin + (size >> (k + 1)) / LINK * (2 if way == dp[-1] else 1)
        ready.append((free[way] + LATENCY, s, k))

    for s in range(streams):
        clock += size / 2e6
        sent(s, 0, clock)
    while ready:
        ready.sort()
        when, s, k = ready.pop(0)
        clock = max(clock, when) + (size >> k) / 2e6
        turns.append((s, k))
        if k + 1 < steps:
            sent(s, k + 1, clock)
    return orders, turns


def quantized(v):
    m = jnp.maximum(jnp.max(jnp.abs(v), axis=0, keepdims=True), 1e-30)
    return jnp.round(v * (TOP / m)).astype(jnp.int32).astype(jnp.int16), m * (1.0 / TOP)


def kernel(cfg, counts_hbm, x_hbm, dy_hbm, out_ref, *scratch):
    n_dp, n_exp, experts, orders, turns, egs, rows_out, cw = cfg
    streams = len(orders)
    steps = len(orders[0])
    it = iter(scratch)
    counts_ref, x_ref, dy_ref, x_own, x_send, x_got, dy_got, lhs, temp = (next(it) for _ in range(9))
    acc = [next(it) for _ in range(streams)]
    send = [next(it) for _ in range(streams)]
    ssend = [next(it) for _ in range(streams)]
    recv = [[next(it) for _ in range(steps)] for _ in range(streams)]
    srecv = [[next(it) for _ in range(steps)] for _ in range(streams)]
    load, tok_s, tok_r, data_s, data_r, scale_s, scale_r = it

    tokens, hid = x_ref.shape
    ffn = dy_ref.shape[1]
    fsh = ffn // n_exp
    me_dp = lax.axis_index("dp")
    me_ex = lax.axis_index("expert")
    core = lax.rem(me_dp, 2)
    mate = me_dp + 1 - 2 * core

    def flip(value, bit):
        own = lax.rem(value // (1 << bit), 2)
        return value + (1 - 2 * own) * (1 << bit)

    def partner(axis, bit):
        return (flip(me_dp, bit), me_ex) if axis == "dp" else (me_dp, flip(me_ex, bit))

    x_load = pltpu.make_async_copy(x_hbm, x_ref, load.at[0])
    dy_load = pltpu.make_async_copy(dy_hbm, dy_ref, load.at[1])
    counts_load = pltpu.make_async_copy(counts_hbm, counts_ref, load.at[2])
    x_load.start()
    counts_load.start()
    dy_load.start()
    barrier = pltpu.get_barrier_semaphore()
    peers = [(mate, me_ex)] + [partner(*d) for d in orders[0]]
    for peer in peers:
        pl.semaphore_signal(barrier, inc=1, device_id=peer, device_id_type=MESH)
    pl.semaphore_wait(barrier, len(peers))

    def remote(src, dst, s_sem, r_sem, peer):
        return pltpu.make_async_remote_copy(
            src_ref=src, dst_ref=dst, send_sem=s_sem, recv_sem=r_sem,
            device_id=peer, device_id_type=MESH,
        )

    parts = streams // 2
    dy_copies = []
    for part in range(parts):
        for y in range(n_exp):
            cols = pl.ds(y * fsh + part * cw, cw)
            n = part * n_exp + y
            dy_copies.append(
                remote(dy_hbm.at[:, cols], dy_got.at[:, cols], tok_s.at[n], tok_r.at[n], (mate, me_ex))
            )
    for copy in dy_copies[:n_exp]:
        copy.start()
    x_load.wait()

    lanes = 128
    per = lanes // (2 * rows_out)

    def turn(j, _):
        xt = x_ref[:, pl.ds(pl.multiple_of(j * lanes, lanes), lanes)].T
        for g in range(per):
            lo = xt[g * 2 * rows_out : g * 2 * rows_out + rows_out]
            hi = xt[g * 2 * rows_out + rows_out : (g + 1) * 2 * rows_out]
            at = pl.ds(pl.multiple_of((j * per + g) * rows_out, rows_out), rows_out)

            @pl.when(core == 0)
            def _():
                x_own[at, :] = lo
                x_send[at, :] = hi

            @pl.when(core == 1)
            def _():
                x_own[at, :] = hi
                x_send[at, :] = lo
        return 0

    lax.fori_loop(0, hid // lanes, turn, 0)
    x_copy = remote(x_send, x_got, tok_s.at[parts * n_exp], tok_r.at[parts * n_exp], (mate, me_ex))
    x_copy.start()
    for copy in dy_copies[n_exp:]:
        copy.start()
    counts_load.wait()
    dy_load.wait()
    x_copy.wait_recv()

    token = lax.broadcasted_iota(jnp.int32, (1, tokens), 1)

    def masked(ref, dp_index, e):
        row = dp_index * n_exp + me_ex
        start = jnp.int32(0)
        for i in range(experts - 1):
            start = start + jnp.where(i < e, counts_ref[i, row], 0)
        low, high = start * BLOCK, (start + counts_ref[e, row]) * BLOCK
        live = jnp.where((token >= low) & (token < high), 1.0, 0.0).astype(jnp.bfloat16)
        return ref[...] * live

    flights = []

    def ship(s, k, src, ssrc, to):
        for pair in (
            remote(ssrc, srecv[s][k], scale_s.at[s, k], scale_r.at[s, k], to),
            remote(src, recv[s][k], data_s.at[s, k], data_r.at[s, k], to),
        ):
            pair.start()
            flights.append((s, k, pair))

    for s in range(streams):
        order = orders[s]
        group, half_col = s % 2, s // 2
        half = 1 << (steps - 1)
        if group == 0:
            for copy in dy_copies[half_col * n_exp : (half_col + 1) * n_exp]:
                copy.wait_recv()

        def per_expert(el, _, s=s, order=order, group=group, half_col=half_col, half=half):
            e = group * egs + el
            if egs > 1 or half_col == 0:
                lhs[2 * group] = masked(x_own, me_dp, e)
                lhs[2 * group + 1] = masked(x_got, mate, e)

            def per_column(ry, _):
                yy = me_ex
                place_y = 0
                for k, (axis, bit) in enumerate(order):
                    if axis == "expert":
                        r = lax.rem(ry // (1 << bit), 2)
                        yy = yy + r * (flip(me_ex, bit) - me_ex)
                        place_y = place_y + r * (1 << (steps - 1 - k))
                col = pl.multiple_of(yy * fsh + half_col * cw, 128)
                temp[...] = jnp.dot(
                    lhs[2 * group], dy_ref[:, pl.ds(col, cw)], preferred_element_type=jnp.float32
                ) + jnp.dot(lhs[2 * group + 1], dy_got[:, pl.ds(col, cw)], preferred_element_type=jnp.float32)

                def per_block(rq, _):
                    qq = me_dp
                    place = place_y
                    for k, (axis, bit) in enumerate(order):
                        if axis == "dp":
                            r = lax.rem(rq // (1 << (bit - 1)), 2)
                            qq = qq + r * (flip(me_dp, bit) - me_dp)
                            place = place + r * (1 << (steps - 1 - k))
                    v = temp[pl.ds(pl.multiple_of((qq // 2) * rows_out, rows_out), rows_out), :]

                    @pl.when(place >= half)
                    def _():
                        q, scale = quantized(v)
                        send[s][(place - half) * egs + el] = q
                        ssend[s][(place - half) * egs + el] = scale

                    @pl.when(place < half)
                    def _():
                        acc[s][place * egs + el] = v
                    return 0

                lax.fori_loop(0, n_dp // 2, per_block, 0, unroll=UNROLL)
                return 0

            lax.fori_loop(0, n_exp, per_column, 0)
            return 0

        lax.fori_loop(0, egs, per_expert, 0)
        ship(s, 0, send[s], ssend[s], partner(*order[0]))

    for s, k in turns:
        upper = (egs << (steps - 1 - k)) // 2
        group, half_col = s % 2, s // 2
        for fs, fk, pair in flights:
            if fs == s and fk == k:
                pair.wait_recv()
        data, scales, total = recv[s][k], srecv[s][k], acc[s]

        def summed(i, data=data, scales=scales, total=total):
            return total[i] + data[i].astype(jnp.float32) * scales[i]

        if k == steps - 1:
            for el in range(egs):
                out_ref[group * egs + el, :, half_col * cw : (half_col + 1) * cw] = summed(el)
            continue

        def forward(i, _, data=data, scales=scales, summed=summed, upper=upper):
            q, scale = quantized(summed(upper + i))
            data[upper + i] = q
            scales[upper + i] = scale
            return 0

        def keep(i, _, total=total, summed=summed):
            total[i] = summed(i)
            return 0

        unroll = min(UNROLL, upper)
        lax.fori_loop(0, upper, forward, 0, unroll=unroll)
        ship(s, k + 1, data.at[pl.ds(upper, upper)], scales.at[pl.ds(upper, upper)], partner(*orders[s][k + 1]))
        lax.fori_loop(0, upper, keep, 0, unroll=unroll)

    for copy in dy_copies:
        copy.wait_send()
    x_copy.wait_send()
    for _, _, pair in flights:
        pair.wait_send()


def shards(n_dp, n_exp, x_rows, dy_rows, seg_blocks):
    tokens, hid = x_rows.shape
    ffn = dy_rows.shape[1]
    experts = seg_blocks.shape[1]
    egs = experts // 2
    rows_out = hid // n_dp
    fsh = ffn // n_exp
    parts = min(PARTS, fsh // 128)
    cw = fsh // parts
    streams = 2 * parts
    orders, turns = plan(n_dp, n_exp, streams, egs * (hid // 2) * n_exp * cw * 2)
    steps = len(orders[0])
    sizes = [(1 << (steps - 1 - k)) * egs for k in range(steps)]
    scratch = [
        pltpu.SMEM(seg_blocks.shape[::-1], seg_blocks.dtype),
        pltpu.VMEM(x_rows.shape, x_rows.dtype),
        pltpu.VMEM(dy_rows.shape, dy_rows.dtype),
        pltpu.VMEM((hid // 2, tokens), x_rows.dtype),
        pltpu.VMEM((hid // 2, tokens), x_rows.dtype),
        pltpu.VMEM((hid // 2, tokens), x_rows.dtype),
        pltpu.VMEM((tokens, ffn), dy_rows.dtype),
        pltpu.VMEM((4, hid // 2, tokens), x_rows.dtype),
        pltpu.VMEM((hid // 2, cw), jnp.float32),
    ]
    scratch += [pltpu.VMEM((sizes[0], rows_out, cw), jnp.float32)] * streams
    scratch += [pltpu.VMEM((sizes[0], rows_out, cw), jnp.int16)] * streams
    scratch += [pltpu.VMEM((sizes[0], 1, cw), jnp.float32)] * streams
    for _ in range(streams):
        scratch += [pltpu.VMEM((size, rows_out, cw), jnp.int16) for size in sizes]
    for _ in range(streams):
        scratch += [pltpu.VMEM((size, 1, cw), jnp.float32) for size in sizes]
    scratch += [pltpu.SemaphoreType.DMA((3,))] + [pltpu.SemaphoreType.DMA((parts * n_exp + 1,))] * 2 + [pltpu.SemaphoreType.DMA((streams, steps))] * 4
    used = sum(math.prod(a.shape) * jnp.dtype(a.dtype).itemsize for a in scratch if a.memory_space == pltpu.VMEM)
    room = min(60 << 20, used + (8 << 20))
    cfg = (n_dp, n_exp, experts, orders, turns, egs, rows_out, cw)
    return pl.pallas_call(
        functools.partial(kernel, cfg),
        out_shape=jax.ShapeDtypeStruct((experts, rows_out, fsh), jnp.float32),
        in_specs=[pl.BlockSpec(memory_space=pl.ANY)] * 3,
        out_specs=pl.BlockSpec(memory_space=pltpu.VMEM),
        scratch_shapes=scratch,
        compiler_params=pltpu.CompilerParams(
            collective_id=0, has_side_effects=True, vmem_limit_bytes=room
        ),
        name="grouped_grad",
    )(*(pltpu.with_memory_space_constraint(a, pltpu.HBM) for a in (seg_blocks.T, x_rows, dy_rows)))


def solution(mesh):
    in_specs = (P(("dp", "expert"), None), P(("dp", "expert"), None), P())
    out_specs = P(None, "dp", "expert")
    body = functools.partial(shards, mesh.shape["dp"], mesh.shape["expert"])
    return jax.shard_map(body, mesh=mesh, in_specs=in_specs, out_specs=out_specs, check_vma=False)
```

```python
import functools
import math

import jax
import jax.numpy as jnp
from jax import lax
from jax.experimental import pallas as pl
from jax.experimental.pallas import tpu as pltpu
from jax.sharding import PartitionSpec as P

BLOCK = 128
CAP = 2
LANES = 128
MESH = pl.DeviceIdType.MESH
TOP = 32767.0
UNROLL = 4
LINK = 46.6e3
LATENCY = 1.9
HOP = 0.6
COMPUTE = 0.55
TURN = 0.2
SPEED = 4e5
PATTERN = (4, 1, 0, 4, 0, 1, 4, 5, 2, 5, 3, 2, 3, 0, 1, 2)


def bits_of(size):
    count = size.bit_length() - 1
    assert size == 1 << count
    return count


def line_of(way):
    axis, bit = way
    if axis != "dp":
        return axis, 1
    return (axis, 1) if bit == 1 else ("far", 1 << (bit - 2))


def plan(n_dp, n_exp, streams, size):
    dp = [("dp", b) for b in range(1, bits_of(n_dp))]
    ex = [("expert", b) for b in range(bits_of(n_exp))]
    x, z, rest = dp[:1], dp[1:2], dp[2:]
    ways = (x + ex + z + rest, ex + x + z + rest, ex + z + x + rest, x + z + ex + rest, z + x + ex + rest, z + ex + x + rest)
    orders = [ways[PATTERN[s % len(PATTERN)]] for s in range(streams)]
    steps = len(orders[0])
    free, flying, turns, clock, first = {}, [], [], 0.0, 0

    def sent(s, k, now):
        line, hops = line_of(orders[s][k])
        free[line] = max(now, free.get(line, 0.0)) + (size >> (k + 1)) / LINK * hops
        flying.append((free[line] + LATENCY + HOP * (hops - 1), s, k))

    while first < streams or flying:
        landed = [(k, when, s) for when, s, k in flying if when <= clock]
        if not landed and first < streams:
            turns.append((first, -1))
            clock += COMPUTE
            sent(first, 0, clock)
            first += 1
            continue
        if landed:
            k, when, s = min(landed)
        else:
            when, s, k = min(flying)
        flying.remove((when, s, k))
        clock = max(clock, when) + TURN + (size >> (k + 1)) / SPEED
        turns.append((s, k))
        if k + 1 < steps:
            sent(s, k + 1, clock)
    return orders, turns


def quantized(v):
    m = jnp.maximum(jnp.max(jnp.abs(v), axis=0, keepdims=True), 1e-30)
    return jnp.round(v * (TOP / m)).astype(jnp.int32).astype(jnp.int16), m * (1.0 / TOP)


def kernel(cfg, counts_hbm, x_hbm, dy_hbm, out_ref, *scratch):
    n_dp, n_exp, experts, orders, turns, egs, rows_out, parts = cfg
    streams = len(orders)
    steps = len(orders[0])
    it = iter(scratch)
    counts_ref, x_ref, x_own, x_send, x_got, lhs, temp = (next(it) for _ in range(7))
    dy_own = [next(it) for _ in range(parts)]
    dy_got = [next(it) for _ in range(parts)]
    acc = [next(it) for _ in range(streams)]
    send = [next(it) for _ in range(streams)]
    ssend = [next(it) for _ in range(streams)]
    recv = [[next(it) for _ in range(steps)] for _ in range(streams)]
    srecv = [[next(it) for _ in range(steps)] for _ in range(streams)]
    load, tok_s, tok_r, data_s, data_r, scale_s, scale_r, ready, go = it

    hid = x_ref.shape[1]
    fsh = dy_hbm.shape[2] // n_exp
    blocks = dy_hbm.shape[0]
    me_dp = lax.axis_index("dp")
    me_ex = lax.axis_index("expert")
    core = lax.rem(me_dp, 2)
    mate = me_dp + 1 - 2 * core

    def flip(value, bit):
        own = lax.rem(value // (1 << bit), 2)
        return value + (1 - 2 * own) * (1 << bit)

    def partner(axis, bit):
        return (flip(me_dp, bit), me_ex) if axis == "dp" else (me_dp, flip(me_ex, bit))

    x_load = pltpu.make_async_copy(x_hbm, x_ref, load.at[0])
    counts_load = pltpu.make_async_copy(counts_hbm, counts_ref, load.at[1])
    x_load.start()
    counts_load.start()
    dy_loads = []
    for part in range(parts):
        for y in range(n_exp):
            dy_loads.append(pltpu.make_async_copy(
                dy_hbm.at[:, :, pl.ds(y * fsh + part * LANES, LANES)],
                dy_own[part].at[:, :, pl.ds(y * LANES, LANES)],
                load.at[2 + part * n_exp + y],
            ))
            dy_loads[-1].start()

    barrier = pltpu.get_barrier_semaphore()
    peers = [partner(*d) for d in orders[0]]

    @pl.when(core == 1)
    def _():
        pl.semaphore_signal(barrier, inc=1, device_id=(mate, me_ex), device_id_type=MESH)

    @pl.when(core == 0)
    def _():
        pl.semaphore_wait(barrier, 1)
        pl.semaphore_signal(ready, inc=1, device_id=(mate, me_ex), device_id_type=MESH)

    @pl.when(core == 1)
    def _():
        pl.semaphore_wait(ready, 1)
        for peer in peers:
            pl.semaphore_signal(barrier, inc=1, device_id=peer, device_id_type=MESH)

    def remote(src, dst, s_sem, r_sem, peer):
        return pltpu.make_async_remote_copy(
            src_ref=src, dst_ref=dst, send_sem=s_sem, recv_sem=r_sem,
            device_id=peer, device_id_type=MESH,
        )

    x_load.wait()
    per = LANES // (2 * rows_out)

    def turn(j, _):
        xt = x_ref[:, pl.ds(pl.multiple_of(j * LANES, LANES), LANES)].T
        for g in range(per):
            lo = xt[g * 2 * rows_out : g * 2 * rows_out + rows_out]
            hi = xt[g * 2 * rows_out + rows_out : (g + 1) * 2 * rows_out]
            at = pl.ds(pl.multiple_of((j * per + g) * rows_out, rows_out), rows_out)

            for b in range(blocks):
                cut = slice(b * BLOCK, (b + 1) * BLOCK)

                @pl.when(core == 0)
                def _():
                    x_own[b, at, :] = lo[:, cut]
                    x_send[b, at, :] = hi[:, cut]

                @pl.when(core == 1)
                def _():
                    x_own[b, at, :] = hi[:, cut]
                    x_send[b, at, :] = lo[:, cut]
        return 0

    lax.fori_loop(0, hid // LANES, turn, 0)
    mate_copies = [remote(x_send, x_got, tok_s.at[parts], tok_r.at[parts], (mate, me_ex))]
    mate_copies[0].start()
    for part in range(parts):
        for y in range(n_exp):
            dy_loads[part * n_exp + y].wait()
        mate_copies.append(remote(dy_own[part], dy_got[part], tok_s.at[part], tok_r.at[part], (mate, me_ex)))
        mate_copies[-1].start()
    counts_load.wait()

    lane = lax.broadcasted_iota(jnp.int32, (1, LANES), 1)

    def segment(dp_index, e):
        row = dp_index * n_exp + me_ex
        start = jnp.int32(0)
        for i in range(experts - 1):
            start = start + jnp.where(i < e, counts_ref[i, row], 0)
        count = counts_ref[e, row]
        return count, [jnp.minimum(start + j, blocks - 1) for j in range(CAP)]

    def packed(ref, dp_index, first):
        def one(e, _):
            count, spots = segment(dp_index, e)
            for j, at in enumerate(spots):
                keep = jnp.where(lane < (count - j) * BLOCK, 1.0, 0.0).astype(jnp.bfloat16)
                lhs[e, :, (first + j) * BLOCK : (first + j + 1) * BLOCK] = ref[at] * keep
            return 0

        lax.fori_loop(0, experts, one, 0)

    packed(x_own, me_dp, 0)
    mate_copies[0].wait_recv()
    packed(x_got, mate, CAP)

    flights = []

    def ship(s, k, src, ssrc, to):
        for pair in (
            remote(ssrc, srecv[s][k], scale_s.at[s, k], scale_r.at[s, k], to),
            remote(src, recv[s][k], data_s.at[s, k], data_r.at[s, k], to),
        ):
            pair.start()
            flights.append((s, k, pair))

    def everyone():
        @pl.when(core == 1)
        def _():
            pl.semaphore_wait(barrier, len(peers))
            pl.semaphore_signal(go, inc=1, device_id=(mate, me_ex), device_id_type=MESH)

        @pl.when(core == 0)
        def _():
            pl.semaphore_wait(go, 1)

    def opening(s):
        order = orders[s]
        group, part = s % 2, s // 2
        half = 1 << (steps - 1)
        if group == 0:
            mate_copies[1 + part].wait_recv()

        def block_of(place):
            qq, yy = me_dp, me_ex
            for k, (axis, bit) in enumerate(order):
                r = lax.rem(place // (1 << (steps - 1 - k)), 2)
                if axis == "dp":
                    qq = qq + r * (flip(me_dp, bit) - me_dp)
                else:
                    yy = yy + r * (flip(me_ex, bit) - me_ex)
            return temp[yy, pl.ds(pl.multiple_of((qq // 2) * rows_out, rows_out), rows_out), :]

        def per_expert(el, _):
            e = group * egs + el
            spots = [(ref, at) for ref, d in ((dy_own[part], me_dp), (dy_got[part], mate)) for at in segment(d, e)[1]]
            wide = min(2, n_exp)
            for y in range(0, n_exp, wide):
                cols = slice(y * LANES, (y + wide) * LANES)
                rhs = jnp.concatenate([ref[at, :, cols] for ref, at in spots], axis=0)
                got = jnp.dot(lhs[e], rhs, preferred_element_type=jnp.float32)
                for w in range(wide):
                    temp[y + w] = got[:, w * LANES : (w + 1) * LANES]

            def away(p, _):
                q, scale = quantized(block_of(half + p))
                send[s][p * egs + el] = q
                ssend[s][p * egs + el] = scale
                return 0

            def home(p, _):
                acc[s][p * egs + el] = block_of(p)
                return 0

            lax.fori_loop(0, half, away, 0, unroll=UNROLL)
            if egs == 1:
                if s == 0:
                    everyone()
                ship(s, 0, send[s], ssend[s], partner(*order[0]))
            lax.fori_loop(0, half, home, 0, unroll=UNROLL)
            return 0

        if egs == 1:
            per_expert(0, 0)
        else:
            lax.fori_loop(0, egs, per_expert, 0)
            if s == 0:
                everyone()
            ship(s, 0, send[s], ssend[s], partner(*order[0]))

    for s, k in turns:
        if k < 0:
            opening(s)
            continue
        upper = (egs << (steps - 1 - k)) // 2
        group, part = s % 2, s // 2
        for fs, fk, pair in flights:
            if fs == s and fk == k:
                pair.wait_recv()
        data, scales, total = recv[s][k], srecv[s][k], acc[s]

        def summed(i, data=data, scales=scales, total=total):
            return total[i] + data[i].astype(jnp.float32) * scales[i]

        if k == steps - 1:
            for el in range(egs):
                out_ref[group * egs + el, :, part * LANES : (part + 1) * LANES] = summed(el)
            continue

        def forward(i, _, data=data, scales=scales, summed=summed, upper=upper):
            q, scale = quantized(summed(upper + i))
            data[upper + i] = q
            scales[upper + i] = scale
            return 0

        def keep(i, _, total=total, summed=summed):
            total[i] = summed(i)
            return 0

        unroll = min(UNROLL, upper)
        lax.fori_loop(0, upper, forward, 0, unroll=unroll)
        ship(s, k + 1, data.at[pl.ds(upper, upper)], scales.at[pl.ds(upper, upper)], partner(*orders[s][k + 1]))
        lax.fori_loop(0, upper, keep, 0, unroll=unroll)

    for copy in mate_copies:
        copy.wait_send()
    for _, _, pair in flights:
        pair.wait_send()


def shards(n_dp, n_exp, x_rows, dy_rows, seg_blocks):
    tokens, hid = x_rows.shape
    ffn = dy_rows.shape[1]
    experts = seg_blocks.shape[1]
    egs = experts // 2
    rows_out = hid // n_dp
    fsh = ffn // n_exp
    parts = fsh // LANES
    streams = 2 * parts
    orders, turns = plan(n_dp, n_exp, streams, egs * (hid // 2) * n_exp * LANES * 2)
    steps = len(orders[0])
    sizes = [(1 << (steps - 1 - k)) * egs for k in range(steps)]
    scratch = [
        pltpu.SMEM(seg_blocks.shape[::-1], seg_blocks.dtype),
        pltpu.VMEM(x_rows.shape, x_rows.dtype),
        pltpu.VMEM((tokens // BLOCK, hid // 2, BLOCK), x_rows.dtype),
        pltpu.VMEM((tokens // BLOCK, hid // 2, BLOCK), x_rows.dtype),
        pltpu.VMEM((tokens // BLOCK, hid // 2, BLOCK), x_rows.dtype),
        pltpu.VMEM((experts, hid // 2, 2 * CAP * BLOCK), x_rows.dtype),
        pltpu.VMEM((n_exp, hid // 2, LANES), jnp.float32),
    ]
    scratch += [pltpu.VMEM((tokens // BLOCK, BLOCK, n_exp * LANES), dy_rows.dtype)] * (2 * parts)
    scratch += [pltpu.VMEM((sizes[0], rows_out, LANES), jnp.float32)] * streams
    scratch += [pltpu.VMEM((sizes[0], rows_out, LANES), jnp.int16)] * streams
    scratch += [pltpu.VMEM((sizes[0], 1, LANES), jnp.float32)] * streams
    for _ in range(streams):
        scratch += [pltpu.VMEM((size, rows_out, LANES), jnp.int16) for size in sizes]
    for _ in range(streams):
        scratch += [pltpu.VMEM((size, 1, LANES), jnp.float32) for size in sizes]
    used = sum(math.prod(a.shape) * jnp.dtype(a.dtype).itemsize for a in scratch if a.memory_space == pltpu.VMEM)
    room = min(60 << 20, used + (8 << 20))
    scratch += [pltpu.SemaphoreType.DMA((2 + parts * n_exp,))] + [pltpu.SemaphoreType.DMA((parts + 1,))] * 2
    scratch += [pltpu.SemaphoreType.DMA((streams, steps))] * 4 + [pltpu.SemaphoreType.REGULAR] * 2
    cfg = (n_dp, n_exp, experts, orders, turns, egs, rows_out, parts)
    return pl.pallas_call(
        functools.partial(kernel, cfg),
        out_shape=jax.ShapeDtypeStruct((experts, rows_out, fsh), jnp.float32),
        in_specs=[pl.BlockSpec(memory_space=pl.ANY)] * 3,
        out_specs=pl.BlockSpec(memory_space=pltpu.VMEM),
        scratch_shapes=scratch,
        compiler_params=pltpu.CompilerParams(
            collective_id=0, has_side_effects=True, vmem_limit_bytes=room
        ),
        name="grouped_grad",
    )(*(pltpu.with_memory_space_constraint(a, pltpu.HBM) for a in (seg_blocks.T, x_rows, dy_rows.reshape(-1, BLOCK, ffn))))


def solution(mesh):
    in_specs = (P(("dp", "expert"), None), P(("dp", "expert"), None), P())
    out_specs = P(None, "dp", "expert")
    body = functools.partial(shards, mesh.shape["dp"], mesh.shape["expert"])
    return jax.shard_map(body, mesh=mesh, in_specs=in_specs, out_specs=out_specs, check_vma=False)
```

```python
import functools
import math

import jax
import jax.numpy as jnp
from jax import lax
from jax.experimental import pallas as pl
from jax.experimental.pallas import tpu as pltpu
from jax.sharding import PartitionSpec as P

BLOCK = 128
CAP = 2
LANES = 128
MESH = pl.DeviceIdType.MESH
TOP = 32767.0
UNROLL = 4
SLICES = 4
SHARE = 4
AHEAD = 1
LINK = 46.6e3
LATENCY = 2.9
HOP = 0.6
COMPUTE = 0.55
TURN = 0.2
SPEED = 4e5
SWAP = {("dp", 1): ("expert", 0), ("expert", 0): ("dp", 1)}
PATTERN = (
    7, 4, 15, 10, 12, 7, 5, 1, 0, 3, 1, 5, 0, 12, 12, 0,
)
TURNS = (
    0, 1, 2, 3, 4, 5, 6, 7, 2, 8, 9, 0, 4, 10, 5, 11, 12, 3, 8, 4,
    7, 13, 14, 15, 8, 7, 9, 0, 10, 5, 2, 12, 14, 13, 1, 8, 11, 10, 15, 7,
    12, 6, 14, 9, 4, 2, 1, 13, 3, 10, 11, 15, 6, 12, 7, 9, 1, 11, 0, 4,
    3, 6, 14, 8, 2, 10, 15, 5, 13, 11, 9, 14, 1, 5, 6, 12, 0, 3, 13, 15,
)


def bits_of(size):
    count = size.bit_length() - 1
    assert size == 1 << count
    return count


def line_of(way):
    axis, bit = way
    if axis != "dp":
        return axis, 1
    return (axis, 1) if bit == 1 else ("far", 1 << (bit - 2))


def plan(n_dp, n_exp, streams, size):
    dp = [("dp", b) for b in range(1, bits_of(n_dp))]
    ex = [("expert", b) for b in range(bits_of(n_exp))]
    x, z, rest = dp[:1], dp[1:2], dp[2:]
    ways = [
        x + ex + z + rest, ex + x + z + rest, ex + z + x + rest, x + z + ex + rest, z + x + ex + rest, z + ex + x + rest,
        x + z + rest + ex, ex + z + rest + x, z + x + rest + ex, z + ex + rest + x, z + rest + x + ex, z + rest + ex + x,
        x + ex + rest + z, ex + x + rest + z, x + rest + ex + z, ex + rest + x + z,
    ]
    orders = [ways[PATTERN[s % len(PATTERN)]] for s in range(streams)]
    steps = len(orders[0])
    if len(TURNS) == streams * (steps + 1):
        count = [-2] * streams
        turns = []
        for s in TURNS:
            count[s] += 1
            turns.append((s, count[s]))
        return orders, turns
    free, flying, turns, clock, first = {}, [], [], 0.0, 0

    def sent(s, k, now):
        line, hops = line_of(orders[s][k])
        free[line] = max(now, free.get(line, 0.0)) + (size >> (k + 1)) / LINK * hops
        flying.append((free[line] + LATENCY + HOP * (hops - 1), s, k))

    while first < streams or flying:
        landed = [(k, when, s) for when, s, k in flying if when <= clock]
        if not landed and first < streams:
            turns.append((first, -1))
            clock += COMPUTE
            sent(first, 0, clock)
            first += 1
            continue
        if landed:
            k, when, s = min(landed)
        else:
            when, s, k = min(flying)
        flying.remove((when, s, k))
        clock = max(clock, when) + TURN + (size >> (k + 1)) / SPEED
        turns.append((s, k))
        if k + 1 < steps:
            sent(s, k + 1, clock)
    return orders, turns


def quantized(values):
    peak = functools.reduce(jnp.maximum, [jnp.abs(v) for v in values])
    m = jnp.maximum(jnp.max(peak, axis=0, keepdims=True), 1e-30)
    return [jnp.round(v * (TOP / m)).astype(jnp.int32).astype(jnp.int16) for v in values], m * (1.0 / TOP)


def kernel(cfg, counts_hbm, x_hbm, dy_hbm, out_ref, *scratch):
    n_dp, n_exp, experts, orders, turns, egs, rows_out, parts = cfg
    streams = len(orders)
    steps = len(orders[0])
    share = SHARE if egs == 1 else 1
    it = iter(scratch)
    counts_ref, x_ref, x_own, x_send, x_got, lhs, temp = (next(it) for _ in range(7))
    dy_own = [next(it) for _ in range(parts)]
    dy_got = [next(it) for _ in range(parts)]
    acc = [next(it) for _ in range(streams)]
    send = [next(it) for _ in range(streams)]
    ssend = [next(it) for _ in range(streams)]
    recv = [[next(it) for _ in range(steps)] for _ in range(streams)]
    srecv = [[next(it) for _ in range(steps)] for _ in range(streams)]
    sfwd = [[next(it) for _ in range(steps - 1)] for _ in range(streams)]
    load, tok_s, tok_r, data_s, data_r, scale_s, scale_r, ready, go = it

    hid = x_ref.shape[1]
    fsh = dy_hbm.shape[2] // n_exp
    blocks = dy_hbm.shape[0]
    me_dp = lax.axis_index("dp")
    me_ex = lax.axis_index("expert")
    core = lax.rem(me_dp, 2)
    mate = me_dp + 1 - 2 * core

    def flip(value, bit):
        own = lax.rem(value // (1 << bit), 2)
        return value + (1 - 2 * own) * (1 << bit)

    def partner(axis, bit):
        return (flip(me_dp, bit), me_ex) if axis == "dp" else (me_dp, flip(me_ex, bit))

    def toward(way):
        dp, ex = partner(*way)
        dp_too, ex_too = partner(*SWAP.get(way, way))
        return dp + core * (dp_too - dp), ex + core * (ex_too - ex)

    wide_x = hid // SLICES
    x_loads = []
    for c in range(SLICES):
        cols = pl.ds(c * wide_x, wide_x)
        x_loads.append(pltpu.make_async_copy(x_hbm.at[:, cols], x_ref.at[:, cols], load.at[1 + c]))
        x_loads[-1].start()
    counts_load = pltpu.make_async_copy(counts_hbm, counts_ref, load.at[0])
    counts_load.start()
    dy_loads = []
    for part in range(parts):
        for y in range(n_exp):
            dy_loads.append(pltpu.make_async_copy(
                dy_hbm.at[:, :, pl.ds(y * fsh + part * LANES, LANES)],
                dy_own[part].at[:, :, pl.ds(y * LANES, LANES)],
                load.at[1 + SLICES + part * n_exp + y],
            ))
            dy_loads[-1].start()

    barrier = pltpu.get_barrier_semaphore()
    peers = [partner(*d) for d in orders[0]]

    @pl.when(core == 1)
    def _():
        pl.semaphore_signal(barrier, inc=1, device_id=(mate, me_ex), device_id_type=MESH)

    def remote(src, dst, s_sem, r_sem, peer):
        return pltpu.make_async_remote_copy(
            src_ref=src, dst_ref=dst, send_sem=s_sem, recv_sem=r_sem,
            device_id=peer, device_id_type=MESH,
        )

    per = LANES // (2 * rows_out)

    def turn(j, _):
        xt = x_ref[:, pl.ds(pl.multiple_of(j * LANES, LANES), LANES)].T
        for g in range(per):
            lo = xt[g * 2 * rows_out : g * 2 * rows_out + rows_out]
            hi = xt[g * 2 * rows_out + rows_out : (g + 1) * 2 * rows_out]
            at = pl.ds(pl.multiple_of((j * per + g) * rows_out, rows_out), rows_out)

            for b in range(blocks):
                cut = slice(b * BLOCK, (b + 1) * BLOCK)

                @pl.when(core == 0)
                def _():
                    x_own[b, at, :] = lo[:, cut]
                    x_send[b, at, :] = hi[:, cut]

                @pl.when(core == 1)
                def _():
                    x_own[b, at, :] = hi[:, cut]
                    x_send[b, at, :] = lo[:, cut]
        return 0


    @pl.when(core == 0)
    def _():
        pl.semaphore_wait(barrier, 1)
        pl.semaphore_signal(ready, inc=1, device_id=(mate, me_ex), device_id_type=MESH)

    @pl.when(core == 1)
    def _():
        pl.semaphore_wait(ready, 1)
        for peer in peers:
            pl.semaphore_signal(barrier, inc=1, device_id=peer, device_id_type=MESH)

    mate_copies = []
    for c in range(SLICES):
        x_loads[c].wait()
        lax.fori_loop(c * wide_x // LANES, (c + 1) * wide_x // LANES, turn, 0)
        at = pl.ds(c * wide_x // 2, wide_x // 2)
        mate_copies.append(remote(x_send.at[:, at], x_got.at[:, at], tok_s.at[c], tok_r.at[c], (mate, me_ex)))
        mate_copies[-1].start()
    for part in range(parts):
        for y in range(n_exp):
            dy_loads[part * n_exp + y].wait()
        mate_copies.append(remote(dy_own[part], dy_got[part], tok_s.at[SLICES + part], tok_r.at[SLICES + part], (mate, me_ex)))
        if part < AHEAD:
            mate_copies[-1].start()
    counts_load.wait()

    lane = lax.broadcasted_iota(jnp.int32, (1, LANES), 1)

    def segment(dp_index, e):
        row = dp_index * n_exp + me_ex
        start = jnp.int32(0)
        for i in range(experts - 1):
            start = start + jnp.where(i < e, counts_ref[i, row], 0)
        count = counts_ref[e, row]
        return count, [jnp.minimum(start + j, blocks - 1) for j in range(CAP)]

    def packed(ref, dp_index, first):
        def one(e, _):
            count, spots = segment(dp_index, e)
            for j, at in enumerate(spots):
                keep = jnp.where(lane < (count - j) * BLOCK, 1.0, 0.0).astype(jnp.bfloat16)
                lhs[e, :, (first + j) * BLOCK : (first + j + 1) * BLOCK] = ref[at] * keep
            return 0

        lax.fori_loop(0, experts, one, 0)

    packed(x_own, me_dp, 0)
    for copy in mate_copies[:SLICES]:
        copy.wait_recv()
    packed(x_got, mate, CAP)

    flights = []

    def ship(s, k, src, ssrc, to):
        for pair in (
            remote(ssrc, srecv[s][k], scale_s.at[s, k], scale_r.at[s, k], to),
            remote(src, recv[s][k], data_s.at[s, k], data_r.at[s, k], to),
        ):
            pair.start()
            flights.append((s, k, pair))

    def everyone():
        @pl.when(core == 1)
        def _():
            pl.semaphore_wait(barrier, len(peers))
            pl.semaphore_signal(go, inc=1, device_id=(mate, me_ex), device_id_type=MESH)

        @pl.when(core == 0)
        def _():
            pl.semaphore_wait(go, 1)

    def opening(s):
        order = orders[s]
        group, part = s % 2, s // 2
        half = 1 << (steps - 1)
        goals = [toward(way) for way in order]
        if group == 0:
            if part + AHEAD < parts:
                mate_copies[SLICES + part + AHEAD].start()
            mate_copies[SLICES + part].wait_recv()

        def block_of(place):
            qq, yy = me_dp, me_ex
            for k, (dp, ex) in enumerate(goals):
                r = lax.rem(place // (1 << (steps - 1 - k)), 2)
                qq = qq + r * (dp - me_dp)
                yy = yy + r * (ex - me_ex)
            return temp[yy, pl.ds(pl.multiple_of((qq // 2) * rows_out, rows_out), rows_out), :]

        def per_expert(el, _):
            e = group * egs + el
            spots = [(ref, at) for ref, d in ((dy_own[part], me_dp), (dy_got[part], mate)) for at in segment(d, e)[1]]
            wide = min(2, n_exp)
            for y in range(0, n_exp, wide):
                cols = slice(y * LANES, (y + wide) * LANES)
                rhs = jnp.concatenate([ref[at, :, cols] for ref, at in spots], axis=0)
                got = jnp.dot(lhs[e], rhs, preferred_element_type=jnp.float32)
                for w in range(wide):
                    temp[y + w] = got[:, w * LANES : (w + 1) * LANES]

            near = min(share, half)

            def away(g, _):
                qs, scale = quantized([block_of(half + g * near + j) for j in range(near)])
                for j, q in enumerate(qs):
                    send[s][(g * near + j) * egs + el] = q
                ssend[s][g * egs + el] = scale
                return 0

            def home(p, _):
                acc[s][p * egs + el] = block_of(p)
                return 0

            lax.fori_loop(0, half // near, away, 0, unroll=UNROLL // near)
            if egs == 1:
                if s == 0:
                    everyone()
                ship(s, 0, send[s], ssend[s], goals[0])
            lax.fori_loop(0, half, home, 0, unroll=UNROLL)
            return 0

        if egs == 1:
            per_expert(0, 0)
        else:
            lax.fori_loop(0, egs, per_expert, 0)
            if s == 0:
                everyone()
            ship(s, 0, send[s], ssend[s], goals[0])

    for s, k in turns:
        if k < 0:
            opening(s)
            continue
        upper = (egs << (steps - 1 - k)) // 2
        group, part = s % 2, s // 2
        for fs, fk, pair in flights:
            if fs == s and fk == k:
                pair.wait_recv()
        data, scales, total = recv[s][k], srecv[s][k], acc[s]

        near = min(share, 2 * upper if k < steps - 1 else egs)

        def summed(i, data=data, scales=scales, total=total, near=near):
            return total[i] + data[i].astype(jnp.float32) * scales[i // near]

        if k == steps - 1:
            for el in range(egs):
                out_ref[group * egs + el, :, part * LANES : (part + 1) * LANES] = summed(el)
            continue

        far = min(share, upper)

        def forward(g, _, data=data, fresh=sfwd[s][k], summed=summed, upper=upper, far=far):
            qs, scale = quantized([summed(upper + g * far + j) for j in range(far)])
            for j, q in enumerate(qs):
                data[upper + g * far + j] = q
            fresh[g] = scale
            return 0

        def keep(i, _, total=total, summed=summed):
            total[i] = summed(i)
            return 0

        unroll = min(UNROLL, upper)
        lax.fori_loop(0, upper // far, forward, 0, unroll=max(1, unroll // far))
        ship(s, k + 1, data.at[pl.ds(upper, upper)], sfwd[s][k], toward(orders[s][k + 1]))
        lax.fori_loop(0, upper, keep, 0, unroll=unroll)

    for copy in mate_copies:
        copy.wait_send()
    for _, _, pair in flights:
        pair.wait_send()


def shards(n_dp, n_exp, x_rows, dy_rows, seg_blocks):
    tokens, hid = x_rows.shape
    ffn = dy_rows.shape[1]
    experts = seg_blocks.shape[1]
    egs = experts // 2
    rows_out = hid // n_dp
    fsh = ffn // n_exp
    parts = fsh // LANES
    streams = 2 * parts
    orders, turns = plan(n_dp, n_exp, streams, egs * (hid // 2) * n_exp * LANES * 2)
    steps = len(orders[0])
    sizes = [(1 << (steps - 1 - k)) * egs for k in range(steps)]
    scratch = [
        pltpu.SMEM(seg_blocks.shape[::-1], seg_blocks.dtype),
        pltpu.VMEM(x_rows.shape, x_rows.dtype),
        pltpu.VMEM((tokens // BLOCK, hid // 2, BLOCK), x_rows.dtype),
        pltpu.VMEM((tokens // BLOCK, hid // 2, BLOCK), x_rows.dtype),
        pltpu.VMEM((tokens // BLOCK, hid // 2, BLOCK), x_rows.dtype),
        pltpu.VMEM((experts, hid // 2, 2 * CAP * BLOCK), x_rows.dtype),
        pltpu.VMEM((n_exp, hid // 2, LANES), jnp.float32),
    ]
    scratch += [pltpu.VMEM((tokens // BLOCK, BLOCK, n_exp * LANES), dy_rows.dtype)] * (2 * parts)
    scratch += [pltpu.VMEM((sizes[0], rows_out, LANES), jnp.float32)] * streams
    scratch += [pltpu.VMEM((sizes[0], rows_out, LANES), jnp.int16)] * streams
    share = SHARE if egs == 1 else 1
    counts = [size // min(share, size) for size in sizes]
    scratch += [pltpu.VMEM((counts[0], 1, LANES), jnp.float32)] * streams
    for _ in range(streams):
        scratch += [pltpu.VMEM((size, rows_out, LANES), jnp.int16) for size in sizes]
    for _ in range(streams):
        scratch += [pltpu.VMEM((count, 1, LANES), jnp.float32) for count in counts]
    for _ in range(streams):
        scratch += [pltpu.VMEM((count, 1, LANES), jnp.float32) for count in counts[1:]]
    used = sum(math.prod(a.shape) * jnp.dtype(a.dtype).itemsize for a in scratch if a.memory_space == pltpu.VMEM)
    room = min(60 << 20, used + (8 << 20))
    scratch += [pltpu.SemaphoreType.DMA((1 + SLICES + parts * n_exp,))] + [pltpu.SemaphoreType.DMA((parts + SLICES,))] * 2
    scratch += [pltpu.SemaphoreType.DMA((streams, steps))] * 4 + [pltpu.SemaphoreType.REGULAR] * 2
    cfg = (n_dp, n_exp, experts, orders, turns, egs, rows_out, parts)
    return pl.pallas_call(
        functools.partial(kernel, cfg),
        out_shape=jax.ShapeDtypeStruct((experts, rows_out, fsh), jnp.float32),
        in_specs=[pl.BlockSpec(memory_space=pl.ANY)] * 3,
        out_specs=pl.BlockSpec(memory_space=pltpu.VMEM),
        scratch_shapes=scratch,
        compiler_params=pltpu.CompilerParams(
            collective_id=0, has_side_effects=True, vmem_limit_bytes=room
        ),
        name="grouped_grad",
    )(*(pltpu.with_memory_space_constraint(a, pltpu.HBM) for a in (seg_blocks.T, x_rows, dy_rows.reshape(-1, BLOCK, ffn))))


def solution(mesh):
    in_specs = (P(("dp", "expert"), None), P(("dp", "expert"), None), P())
    out_specs = P(None, "dp", "expert")
    body = functools.partial(shards, mesh.shape["dp"], mesh.shape["expert"])
    return jax.shard_map(body, mesh=mesh, in_specs=in_specs, out_specs=out_specs, check_vma=False)
```

```python
import functools
import math

import jax
import jax.numpy as jnp
from jax import lax
from jax.experimental import pallas as pl
from jax.experimental.pallas import tpu as pltpu
from jax.sharding import PartitionSpec as P

BLOCK = 128
CAP = 2
LANES = 128
MESH = pl.DeviceIdType.MESH
TOP = 32767.0
UNROLL = 4
SLICES = 4
SHARE = 4
AHEAD = 1
LINK = 46.6e3
LATENCY = 2.9
HOP = 0.6
COMPUTE = 0.55
TURN = 0.2
SPEED = 4e5
SWAP = {("dp", 1): ("expert", 0), ("expert", 0): ("dp", 1)}
PATTERN = (
    14, 8, 12, 1, 4, 15, 1, 13, 10, 15, 13, 2, 4, 13, 3, 0,
)
TURNS = (
    0, 1, 2, 3, 4, 5, 6, 0, 7, 8, 9, 10, 5, 11, 12, 13, 9, 2, 10, 8,
    14, 11, 7, 15, 10, 6, 2, 13, 14, 3, 1, 7, 4, 12, 9, 15, 6, 13, 11, 3,
    1, 5, 14, 10, 15, 6, 4, 12, 8, 7, 0, 3, 14, 11, 9, 13, 4, 5, 15, 1,
    12, 2, 0, 8, 3, 10, 4, 7, 5, 1, 6, 14, 2, 9, 13, 11, 15, 8, 0, 12,
)


def bits_of(size):
    count = size.bit_length() - 1
    assert size == 1 << count
    return count


def line_of(way):
    axis, bit = way
    if axis != "dp":
        return axis, 1
    return (axis, 1) if bit == 1 else ("far", 1 << (bit - 2))


def plan(n_dp, n_exp, streams, size):
    dp = [("dp", b) for b in range(1, bits_of(n_dp))]
    ex = [("expert", b) for b in range(bits_of(n_exp))]
    x, z, rest = dp[:1], dp[1:2], dp[2:]
    ways = [
        x + ex + z + rest, ex + x + z + rest, ex + z + x + rest, x + z + ex + rest, z + x + ex + rest, z + ex + x + rest,
        x + z + rest + ex, ex + z + rest + x, z + x + rest + ex, z + ex + rest + x, z + rest + x + ex, z + rest + ex + x,
        x + ex + rest + z, ex + x + rest + z, x + rest + ex + z, ex + rest + x + z,
    ]
    orders = [ways[PATTERN[s % len(PATTERN)]] for s in range(streams)]
    steps = len(orders[0])
    if len(TURNS) == streams * (steps + 1):
        count = [-2] * streams
        turns = []
        for s in TURNS:
            count[s] += 1
            turns.append((s, count[s]))
        return orders, turns
    free, flying, turns, clock, first = {}, [], [], 0.0, 0

    def sent(s, k, now):
        line, hops = line_of(orders[s][k])
        free[line] = max(now, free.get(line, 0.0)) + (size >> (k + 1)) / LINK * hops
        flying.append((free[line] + LATENCY + HOP * (hops - 1), s, k))

    while first < streams or flying:
        landed = [(k, when, s) for when, s, k in flying if when <= clock]
        if not landed and first < streams:
            turns.append((first, -1))
            clock += COMPUTE
            sent(first, 0, clock)
            first += 1
            continue
        if landed:
            k, when, s = min(landed)
        else:
            when, s, k = min(flying)
        flying.remove((when, s, k))
        clock = max(clock, when) + TURN + (size >> (k + 1)) / SPEED
        turns.append((s, k))
        if k + 1 < steps:
            sent(s, k + 1, clock)
    return orders, turns


def quantized(values):
    peak = functools.reduce(jnp.maximum, [jnp.abs(v) for v in values])
    m = jnp.maximum(jnp.max(peak, axis=0, keepdims=True), 1e-30)
    return [jnp.round(v * (TOP / m)).astype(jnp.int32).astype(jnp.int16) for v in values], m * (1.0 / TOP)


def kernel(cfg, counts_hbm, x_hbm, dy_hbm, out_ref, *scratch):
    n_dp, n_exp, experts, orders, turns, egs, rows_out, parts = cfg
    streams = len(orders)
    steps = len(orders[0])
    share = SHARE if egs == 1 else 1
    it = iter(scratch)
    counts_ref, x_ref, x_own, x_send, x_got, lhs, temp = (next(it) for _ in range(7))
    dy_own = [next(it) for _ in range(parts)]
    dy_got = [next(it) for _ in range(parts)]
    acc = [next(it) for _ in range(streams)]
    send = [next(it) for _ in range(streams)]
    ssend = [next(it) for _ in range(streams)]
    recv = [[next(it) for _ in range(steps)] for _ in range(streams)]
    srecv = [[next(it) for _ in range(steps)] for _ in range(streams)]
    sfwd = [[next(it) for _ in range(steps - 1)] for _ in range(streams)]
    tally, load, tok_s, tok_r, sent, landed, ready, go = it

    hid = x_ref.shape[1]
    fsh = dy_hbm.shape[2] // n_exp
    blocks = dy_hbm.shape[0]
    me_dp = lax.axis_index("dp")
    me_ex = lax.axis_index("expert")
    core = lax.rem(me_dp, 2)
    mate = me_dp + 1 - 2 * core

    def flip(value, bit):
        own = lax.rem(value // (1 << bit), 2)
        return value + (1 - 2 * own) * (1 << bit)

    def partner(axis, bit):
        return (flip(me_dp, bit), me_ex) if axis == "dp" else (me_dp, flip(me_ex, bit))

    def toward(way):
        dp, ex = partner(*way)
        dp_too, ex_too = partner(*SWAP.get(way, way))
        return dp + core * (dp_too - dp), ex + core * (ex_too - ex)

    wide_x = hid // SLICES
    x_loads = []
    for c in range(SLICES):
        cols = pl.ds(c * wide_x, wide_x)
        x_loads.append(pltpu.make_async_copy(x_hbm.at[:, cols], x_ref.at[:, cols], load.at[1 + c]))
        x_loads[-1].start()
    counts_load = pltpu.make_async_copy(counts_hbm, counts_ref, load.at[0])
    counts_load.start()
    dy_loads = []
    for part in range(parts):
        for y in range(n_exp):
            dy_loads.append(pltpu.make_async_copy(
                dy_hbm.at[:, :, pl.ds(y * fsh + part * LANES, LANES)],
                dy_own[part].at[:, :, pl.ds(y * LANES, LANES)],
                load.at[1 + SLICES + part],
            ))
            dy_loads[-1].start()

    barrier = pltpu.get_barrier_semaphore()
    peers = [partner(*d) for d in orders[0]]

    @pl.when(core == 1)
    def _():
        pl.semaphore_signal(barrier, inc=1, device_id=(mate, me_ex), device_id_type=MESH)

    def remote(src, dst, s_sem, r_sem, peer):
        return pltpu.make_async_remote_copy(
            src_ref=src, dst_ref=dst, send_sem=s_sem, recv_sem=r_sem,
            device_id=peer, device_id_type=MESH,
        )

    per = LANES // (2 * rows_out)

    def turn(j, _):
        xt = x_ref[:, pl.ds(pl.multiple_of(j * LANES, LANES), LANES)].T
        for g in range(per):
            lo = xt[g * 2 * rows_out : g * 2 * rows_out + rows_out]
            hi = xt[g * 2 * rows_out + rows_out : (g + 1) * 2 * rows_out]
            at = pl.ds(pl.multiple_of((j * per + g) * rows_out, rows_out), rows_out)

            for b in range(blocks):
                cut = slice(b * BLOCK, (b + 1) * BLOCK)

                @pl.when(core == 0)
                def _():
                    x_own[b, at, :] = lo[:, cut]
                    x_send[b, at, :] = hi[:, cut]

                @pl.when(core == 1)
                def _():
                    x_own[b, at, :] = hi[:, cut]
                    x_send[b, at, :] = lo[:, cut]
        return 0


    @pl.when(core == 0)
    def _():
        pl.semaphore_wait(barrier, 1)
        pl.semaphore_signal(ready, inc=1, device_id=(mate, me_ex), device_id_type=MESH)

    @pl.when(core == 1)
    def _():
        pl.semaphore_wait(ready, 1)
        for peer in peers:
            pl.semaphore_signal(barrier, inc=1, device_id=peer, device_id_type=MESH)

    mate_copies = []
    for c in range(SLICES):
        x_loads[c].wait()
        lax.fori_loop(c * wide_x // LANES, (c + 1) * wide_x // LANES, turn, 0)
        at = pl.ds(c * wide_x // 2, wide_x // 2)
        mate_copies.append(remote(x_send.at[:, at], x_got.at[:, at], tok_s.at[c], tok_r.at[c], (mate, me_ex)))
        mate_copies[-1].start()
    for part in range(parts):
        pltpu.make_async_copy(dy_own[part], dy_own[part], load.at[1 + SLICES + part]).wait()
        mate_copies.append(remote(dy_own[part], dy_got[part], tok_s.at[SLICES + part], tok_r.at[SLICES + part], (mate, me_ex)))
        if part < AHEAD:
            mate_copies[-1].start()
    counts_load.wait()

    lane = lax.broadcasted_iota(jnp.int32, (1, LANES), 1)

    def segment(dp_index, e):
        row = dp_index * n_exp + me_ex
        start = jnp.int32(0)
        for i in range(experts - 1):
            start = start + jnp.where(i < e, counts_ref[i, row], 0)
        count = counts_ref[e, row]
        return count, [jnp.minimum(start + j, blocks - 1) for j in range(CAP)]

    def packed(ref, dp_index, first):
        def one(e, _):
            count, spots = segment(dp_index, e)
            for j, at in enumerate(spots):
                keep = jnp.where(lane < (count - j) * BLOCK, 1.0, 0.0).astype(jnp.bfloat16)
                lhs[e, :, (first + j) * BLOCK : (first + j + 1) * BLOCK] = ref[at] * keep
            return 0

        lax.fori_loop(0, experts, one, 0)

    packed(x_own, me_dp, 0)
    for copy in mate_copies[:SLICES]:
        copy.wait_recv()
    packed(x_got, mate, CAP)

    sizes = [ref.shape[0] for ref in recv[0]]
    rows_of = [size * rows_out // 2 + ref.shape[0] for size, ref in zip(sizes, srecv[0])]

    def bytes_of(rows, s, k):
        view = tally.at[pl.ds(0, rows)]
        return remote(view, view, sent.at[s], landed.at[s, k], (mate, me_ex))

    def ship(s, k, src, ssrc, to):
        for pair in (
            remote(ssrc, srecv[s][k], sent.at[s], landed.at[s, k], to),
            remote(src, recv[s][k], sent.at[s], landed.at[s, k], to),
        ):
            pair.start()

    def everyone():
        @pl.when(core == 1)
        def _():
            pl.semaphore_wait(barrier, len(peers))
            pl.semaphore_signal(go, inc=1, device_id=(mate, me_ex), device_id_type=MESH)

        @pl.when(core == 0)
        def _():
            pl.semaphore_wait(go, 1)

    def opening(s):
        order = orders[s]
        group, part = s % 2, s // 2
        half = 1 << (steps - 1)
        goals = [toward(way) for way in order]
        if group == 0:
            if part + AHEAD < parts:
                mate_copies[SLICES + part + AHEAD].start()
            mate_copies[SLICES + part].wait_recv()

        def block_of(place):
            qq, yy = me_dp, me_ex
            for k, (dp, ex) in enumerate(goals):
                r = lax.rem(place // (1 << (steps - 1 - k)), 2)
                qq = qq + r * (dp - me_dp)
                yy = yy + r * (ex - me_ex)
            return temp[yy, pl.ds(pl.multiple_of((qq // 2) * rows_out, rows_out), rows_out), :]

        def per_expert(el, _):
            e = group * egs + el
            spots = [(ref, at) for ref, d in ((dy_own[part], me_dp), (dy_got[part], mate)) for at in segment(d, e)[1]]
            wide = min(2, n_exp)
            for y in range(0, n_exp, wide):
                cols = slice(y * LANES, (y + wide) * LANES)
                rhs = jnp.concatenate([ref[at, :, cols] for ref, at in spots], axis=0)
                got = jnp.dot(lhs[e], rhs, preferred_element_type=jnp.float32)
                for w in range(wide):
                    temp[y + w] = got[:, w * LANES : (w + 1) * LANES]

            near = min(share, half)

            def away(g, _):
                qs, scale = quantized([block_of(half + g * near + j) for j in range(near)])
                for j, q in enumerate(qs):
                    send[s][(g * near + j) * egs + el] = q
                ssend[s][g * egs + el] = scale
                return 0

            def home(p, _):
                acc[s][p * egs + el] = block_of(p)
                return 0

            lax.fori_loop(0, half // near, away, 0, unroll=UNROLL // near)
            if egs == 1:
                if s == 0:
                    everyone()
                ship(s, 0, send[s], ssend[s], goals[0])
            lax.fori_loop(0, half, home, 0, unroll=UNROLL)
            return 0

        if egs == 1:
            per_expert(0, 0)
        else:
            lax.fori_loop(0, egs, per_expert, 0)
            if s == 0:
                everyone()
            ship(s, 0, send[s], ssend[s], goals[0])

    for s, k in turns:
        if k < 0:
            opening(s)
            continue
        upper = (egs << (steps - 1 - k)) // 2
        group, part = s % 2, s // 2
        bytes_of(rows_of[k], s, k).wait_recv()
        data, scales, total = recv[s][k], srecv[s][k], acc[s]

        near = min(share, 2 * upper if k < steps - 1 else egs)

        def summed(i, data=data, scales=scales, total=total, near=near):
            return total[i] + data[i].astype(jnp.float32) * scales[i // near]

        if k == steps - 1:
            for el in range(egs):
                out_ref[group * egs + el, :, part * LANES : (part + 1) * LANES] = summed(el)
            continue

        far = min(share, upper)

        def forward(g, _, data=data, fresh=sfwd[s][k], summed=summed, upper=upper, far=far):
            qs, scale = quantized([summed(upper + g * far + j) for j in range(far)])
            for j, q in enumerate(qs):
                data[upper + g * far + j] = q
            fresh[g] = scale
            return 0

        def keep(i, _, total=total, summed=summed):
            total[i] = summed(i)
            return 0

        unroll = min(UNROLL, upper)
        lax.fori_loop(0, upper // far, forward, 0, unroll=max(1, unroll // far))
        ship(s, k + 1, data.at[pl.ds(upper, upper)], sfwd[s][k], toward(orders[s][k + 1]))
        lax.fori_loop(0, upper, keep, 0, unroll=unroll)

    for copy in mate_copies:
        copy.wait_send()
    for s in range(streams):
        bytes_of(sum(rows_of), s, 0).wait_send()


def shards(n_dp, n_exp, x_rows, dy_rows, seg_blocks):
    tokens, hid = x_rows.shape
    ffn = dy_rows.shape[1]
    experts = seg_blocks.shape[1]
    egs = experts // 2
    rows_out = hid // n_dp
    fsh = ffn // n_exp
    parts = fsh // LANES
    streams = 2 * parts
    orders, turns = plan(n_dp, n_exp, streams, egs * (hid // 2) * n_exp * LANES * 2)
    steps = len(orders[0])
    sizes = [(1 << (steps - 1 - k)) * egs for k in range(steps)]
    scratch = [
        pltpu.SMEM(seg_blocks.shape[::-1], seg_blocks.dtype),
        pltpu.VMEM(x_rows.shape, x_rows.dtype),
        pltpu.VMEM((tokens // BLOCK, hid // 2, BLOCK), x_rows.dtype),
        pltpu.VMEM((tokens // BLOCK, hid // 2, BLOCK), x_rows.dtype),
        pltpu.VMEM((tokens // BLOCK, hid // 2, BLOCK), x_rows.dtype),
        pltpu.VMEM((experts, hid // 2, 2 * CAP * BLOCK), x_rows.dtype),
        pltpu.VMEM((n_exp, hid // 2, LANES), jnp.float32),
    ]
    scratch += [pltpu.VMEM((tokens // BLOCK, BLOCK, n_exp * LANES), dy_rows.dtype)] * (2 * parts)
    scratch += [pltpu.VMEM((sizes[0], rows_out, LANES), jnp.float32)] * streams
    scratch += [pltpu.VMEM((sizes[0], rows_out, LANES), jnp.int16)] * streams
    share = SHARE if egs == 1 else 1
    counts = [size // min(share, size) for size in sizes]
    scratch += [pltpu.VMEM((counts[0], 1, LANES), jnp.float32)] * streams
    for _ in range(streams):
        scratch += [pltpu.VMEM((size, rows_out, LANES), jnp.int16) for size in sizes]
    for _ in range(streams):
        scratch += [pltpu.VMEM((count, 1, LANES), jnp.float32) for count in counts]
    for _ in range(streams):
        scratch += [pltpu.VMEM((count, 1, LANES), jnp.float32) for count in counts[1:]]
    scratch += [pltpu.VMEM((sum(sizes) * rows_out // 2 + sum(counts), 1, LANES), jnp.float32)]
    used = sum(math.prod(a.shape) * jnp.dtype(a.dtype).itemsize for a in scratch if a.memory_space == pltpu.VMEM)
    room = min(60 << 20, used + (8 << 20))
    scratch += [pltpu.SemaphoreType.DMA((1 + SLICES + parts,))] + [pltpu.SemaphoreType.DMA((parts + SLICES,))] * 2
    scratch += [pltpu.SemaphoreType.DMA((streams,)), pltpu.SemaphoreType.DMA((streams, steps))] + [pltpu.SemaphoreType.REGULAR] * 2
    cfg = (n_dp, n_exp, experts, orders, turns, egs, rows_out, parts)
    return pl.pallas_call(
        functools.partial(kernel, cfg),
        out_shape=jax.ShapeDtypeStruct((experts, rows_out, fsh), jnp.float32),
        in_specs=[pl.BlockSpec(memory_space=pl.ANY)] * 3,
        out_specs=pl.BlockSpec(memory_space=pltpu.VMEM),
        scratch_shapes=scratch,
        compiler_params=pltpu.CompilerParams(
            collective_id=0, has_side_effects=True, vmem_limit_bytes=room
        ),
        name="grouped_grad",
    )(*(pltpu.with_memory_space_constraint(a, pltpu.HBM) for a in (seg_blocks.T, x_rows, dy_rows.reshape(-1, BLOCK, ffn))))


def solution(mesh):
    in_specs = (P(("dp", "expert"), None), P(("dp", "expert"), None), P())
    out_specs = P(None, "dp", "expert")
    body = functools.partial(shards, mesh.shape["dp"], mesh.shape["expert"])
    return jax.shard_map(body, mesh=mesh, in_specs=in_specs, out_specs=out_specs, check_vma=False)
```

```python
import functools
import math

import jax
import jax.numpy as jnp
from jax import lax
from jax.experimental import pallas as pl
from jax.experimental.pallas import tpu as pltpu
from jax.sharding import PartitionSpec as P

BLOCK = 128
CAP = 2
LANES = 128
MESH = pl.DeviceIdType.MESH
TOP = 32767.0
UNROLL = 4
FLAT = 16
SLICES = 4
SHARE = 4
AHEAD = 1
LINK = 46.6e3
LATENCY = 2.9
HOP = 0.6
COMPUTE = 0.55
TURN = 0.2
SPEED = 4e5
SWAP = {("dp", 1): ("expert", 0), ("expert", 0): ("dp", 1)}
PATTERN = (
    15, 10, 15, 1, 10, 13, 13, 0, 15, 13, 4, 12, 2, 1, 1, 4,
)
TURNS = (
    0, 1, 2, 3, 4, 5, 6, 0, 2, 7, 8, 9, 10, 11, 5, 1, 12, 3, 13, 14,
    15, 6, 4, 8, 5, 7, 11, 12, 13, 9, 15, 14, 3, 10, 6, 7, 13, 2, 11, 4,
    0, 9, 15, 1, 14, 12, 3, 7, 10, 6, 13, 8, 11, 15, 12, 1, 2, 10, 4, 14,
    0, 9, 8, 5, 15, 2, 7, 4, 1, 3, 12, 10, 9, 11, 8, 6, 14, 13, 0, 5,
)


def bits_of(size):
    count = size.bit_length() - 1
    assert size == 1 << count
    return count


def line_of(way):
    axis, bit = way
    if axis != "dp":
        return axis, 1
    return (axis, 1) if bit == 1 else ("far", 1 << (bit - 2))


def plan(n_dp, n_exp, streams, size):
    dp = [("dp", b) for b in range(1, bits_of(n_dp))]
    ex = [("expert", b) for b in range(bits_of(n_exp))]
    x, z, rest = dp[:1], dp[1:2], dp[2:]
    ways = [
        x + ex + z + rest, ex + x + z + rest, ex + z + x + rest, x + z + ex + rest, z + x + ex + rest, z + ex + x + rest,
        x + z + rest + ex, ex + z + rest + x, z + x + rest + ex, z + ex + rest + x, z + rest + x + ex, z + rest + ex + x,
        x + ex + rest + z, ex + x + rest + z, x + rest + ex + z, ex + rest + x + z,
    ]
    orders = [ways[PATTERN[s % len(PATTERN)]] for s in range(streams)]
    steps = len(orders[0])
    if len(TURNS) == streams * (steps + 1):
        count = [-2] * streams
        turns = []
        for s in TURNS:
            count[s] += 1
            turns.append((s, count[s]))
        return orders, turns
    free, flying, turns, clock, first = {}, [], [], 0.0, 0

    def sent(s, k, now):
        line, hops = line_of(orders[s][k])
        free[line] = max(now, free.get(line, 0.0)) + (size >> (k + 1)) / LINK * hops
        flying.append((free[line] + LATENCY + HOP * (hops - 1), s, k))

    while first < streams or flying:
        landed = [(k, when, s) for when, s, k in flying if when <= clock]
        if not landed and first < streams:
            turns.append((first, -1))
            clock += COMPUTE
            sent(first, 0, clock)
            first += 1
            continue
        if landed:
            k, when, s = min(landed)
        else:
            when, s, k = min(flying)
        flying.remove((when, s, k))
        clock = max(clock, when) + TURN + (size >> (k + 1)) / SPEED
        turns.append((s, k))
        if k + 1 < steps:
            sent(s, k + 1, clock)
    return orders, turns


def quantized(values):
    peak = functools.reduce(jnp.maximum, [jnp.abs(v) for v in values])
    m = jnp.maximum(jnp.max(peak, axis=0, keepdims=True), 1e-30)
    return [jnp.round(v * (TOP / m)).astype(jnp.int32).astype(jnp.int16) for v in values], m * (1.0 / TOP)


def kernel(cfg, counts_hbm, x_hbm, dy_hbm, out_ref, *scratch):
    n_dp, n_exp, experts, orders, turns, egs, rows_out, parts = cfg
    streams = len(orders)
    steps = len(orders[0])
    share = SHARE if egs == 1 else 1
    it = iter(scratch)
    counts_ref, x_ref, x_half, x_got, lhs, temp = (next(it) for _ in range(6))
    dy_own = [next(it) for _ in range(parts)]
    dy_got = [next(it) for _ in range(parts)]
    acc = [next(it) for _ in range(streams)]
    send = [next(it) for _ in range(streams)]
    ssend = [next(it) for _ in range(streams)]
    recv = [[next(it) for _ in range(steps)] for _ in range(streams)]
    srecv = [[next(it) for _ in range(steps)] for _ in range(streams)]
    sfwd = [[next(it) for _ in range(steps - 1)] for _ in range(streams)]
    tally, load, tok_s, tok_r, sent, landed, ready, go = it

    hid = x_ref.shape[1]
    fsh = dy_hbm.shape[2] // n_exp
    blocks = dy_hbm.shape[0]
    me_dp = lax.axis_index("dp")
    me_ex = lax.axis_index("expert")
    core = lax.rem(me_dp, 2)
    mate = me_dp + 1 - 2 * core

    def flip(value, bit):
        own = lax.rem(value // (1 << bit), 2)
        return value + (1 - 2 * own) * (1 << bit)

    def partner(axis, bit):
        return (flip(me_dp, bit), me_ex) if axis == "dp" else (me_dp, flip(me_ex, bit))

    def toward(way):
        dp, ex = partner(*way)
        dp_too, ex_too = partner(*SWAP.get(way, way))
        return dp + core * (dp_too - dp), ex + core * (ex_too - ex)

    wide_x = hid // SLICES
    x_loads = []
    for c in range(SLICES):
        cols = pl.ds(c * wide_x, wide_x)
        x_loads.append(pltpu.make_async_copy(x_hbm.at[:, cols], x_ref.at[:, cols], load.at[1 + c]))
        x_loads[-1].start()
    counts_load = pltpu.make_async_copy(counts_hbm, counts_ref, load.at[0])
    counts_load.start()
    dy_loads = []
    for part in range(parts):
        for y in range(n_exp):
            dy_loads.append(pltpu.make_async_copy(
                dy_hbm.at[:, :, pl.ds(y * fsh + part * LANES, LANES)],
                dy_own[part].at[:, :, pl.ds(y * LANES, LANES)],
                load.at[1 + SLICES + part],
            ))
            dy_loads[-1].start()

    barrier = pltpu.get_barrier_semaphore()
    peers = [partner(*d) for d in orders[0]]

    @pl.when(core == 1)
    def _():
        pl.semaphore_signal(barrier, inc=1, device_id=(mate, me_ex), device_id_type=MESH)

    def remote(src, dst, s_sem, r_sem, peer):
        return pltpu.make_async_remote_copy(
            src_ref=src, dst_ref=dst, send_sem=s_sem, recv_sem=r_sem,
            device_id=peer, device_id_type=MESH,
        )

    per = LANES // (2 * rows_out)

    def turn(j, _):
        xt = x_ref[:, pl.ds(pl.multiple_of(j * LANES, LANES), LANES)].T
        for g in range(per):
            lo = xt[g * 2 * rows_out : g * 2 * rows_out + rows_out]
            hi = xt[g * 2 * rows_out + rows_out : (g + 1) * 2 * rows_out]
            at = pl.ds(pl.multiple_of((j * per + g) * rows_out, rows_out), rows_out)

            for b in range(blocks):
                cut = slice(b * BLOCK, (b + 1) * BLOCK)
                x_half[core, b, at, :] = lo[:, cut]
                x_half[1 - core, b, at, :] = hi[:, cut]
        return 0


    @pl.when(core == 0)
    def _():
        pl.semaphore_wait(barrier, 1)
        pl.semaphore_signal(ready, inc=1, device_id=(mate, me_ex), device_id_type=MESH)

    @pl.when(core == 1)
    def _():
        pl.semaphore_wait(ready, 1)
        for peer in peers:
            pl.semaphore_signal(barrier, inc=1, device_id=peer, device_id_type=MESH)

    mate_copies = []
    for c in range(SLICES):
        x_loads[c].wait()
        lax.fori_loop(c * wide_x // LANES, (c + 1) * wide_x // LANES, turn, 0, unroll=wide_x // LANES)
        at = pl.ds(c * wide_x // 2, wide_x // 2)
        mate_copies.append(remote(x_half.at[1, :, at], x_got.at[:, at], tok_s.at[0], tok_r.at[parts], (mate, me_ex)))
        mate_copies[-1].start()
    for part in range(parts):
        pltpu.make_async_copy(dy_own[part], dy_own[part], load.at[1 + SLICES + part]).wait()
        mate_copies.append(remote(dy_own[part], dy_got[part], tok_s.at[1], tok_r.at[part], (mate, me_ex)))
        if part < AHEAD:
            mate_copies[-1].start()
    counts_load.wait()

    lane = lax.broadcasted_iota(jnp.int32, (1, LANES), 1)

    def segment(dp_index, e):
        row = dp_index * n_exp + me_ex
        start = jnp.int32(0)
        for i in range(experts - 1):
            start = start + jnp.where(i < e, counts_ref[i, row], 0)
        count = counts_ref[e, row]
        return count, [jnp.minimum(start + j, blocks - 1) for j in range(CAP)]

    def packed(ref, dp_index, first):
        def one(e, _):
            count, spots = segment(dp_index, e)
            for j, at in enumerate(spots):
                keep = jnp.where(lane < (count - j) * BLOCK, 1.0, 0.0).astype(jnp.bfloat16)
                lhs[e, :, (first + j) * BLOCK : (first + j + 1) * BLOCK] = ref[at] * keep
            return 0

        lax.fori_loop(0, experts, one, 0)

    packed(x_half.at[0], me_dp, 0)
    x_swap = remote(x_half.at[1], x_got, tok_s.at[0], tok_r.at[parts], (mate, me_ex))
    x_swap.wait_recv()
    packed(x_got, mate, CAP)

    sizes = [ref.shape[0] for ref in recv[0]]
    rows_of = [size * rows_out // 2 + ref.shape[0] for size, ref in zip(sizes, srecv[0])]

    def bytes_of(rows, s, k):
        view = tally.at[pl.ds(0, rows)]
        return remote(view, view, sent.at[s], landed.at[s, k], (mate, me_ex))

    def ship(s, k, src, ssrc, to):
        for pair in (
            remote(ssrc, srecv[s][k], sent.at[s], landed.at[s, k], to),
            remote(src, recv[s][k], sent.at[s], landed.at[s, k], to),
        ):
            pair.start()

    def everyone():
        @pl.when(core == 1)
        def _():
            pl.semaphore_wait(barrier, len(peers))
            pl.semaphore_signal(go, inc=1, device_id=(mate, me_ex), device_id_type=MESH)

        @pl.when(core == 0)
        def _():
            pl.semaphore_wait(go, 1)

    def opening(s):
        order = orders[s]
        group, part = s % 2, s // 2
        half = 1 << (steps - 1)
        goals = [toward(way) for way in order]
        if group == 0:
            if part + AHEAD < parts:
                mate_copies[SLICES + part + AHEAD].start()
            mate_copies[SLICES + part].wait_recv()

        def block_of(place):
            qq, yy = me_dp, me_ex
            for k, (dp, ex) in enumerate(goals):
                r = lax.rem(place // (1 << (steps - 1 - k)), 2)
                qq = qq + r * (dp - me_dp)
                yy = yy + r * (ex - me_ex)
            return temp[yy, pl.ds(pl.multiple_of((qq // 2) * rows_out, rows_out), rows_out), :]

        def per_expert(el, _):
            e = group * egs + el
            spots = [(ref, at) for ref, d in ((dy_own[part], me_dp), (dy_got[part], mate)) for at in segment(d, e)[1]]
            wide = min(2, n_exp)
            for y in range(0, n_exp, wide):
                cols = slice(y * LANES, (y + wide) * LANES)
                rhs = jnp.concatenate([ref[at, :, cols] for ref, at in spots], axis=0)
                got = jnp.dot(lhs[e], rhs, preferred_element_type=jnp.float32)
                for w in range(wide):
                    temp[y + w] = got[:, w * LANES : (w + 1) * LANES]

            near = min(share, half)

            def away(g, _):
                qs, scale = quantized([block_of(half + g * near + j) for j in range(near)])
                for j, q in enumerate(qs):
                    send[s][(g * near + j) * egs + el] = q
                ssend[s][g * egs + el] = scale
                return 0

            def home(p, _):
                acc[s][p * egs + el] = block_of(p)
                return 0

            lax.fori_loop(0, half // near, away, 0, unroll=half // near if half <= FLAT else 1)
            if egs == 1:
                if s == 0:
                    everyone()
                ship(s, 0, send[s], ssend[s], goals[0])
            lax.fori_loop(0, half, home, 0, unroll=half if half <= FLAT else UNROLL)
            return 0

        if egs == 1:
            per_expert(0, 0)
        else:
            lax.fori_loop(0, egs, per_expert, 0)
            if s == 0:
                everyone()
            ship(s, 0, send[s], ssend[s], goals[0])

    for s, k in turns:
        if k < 0:
            opening(s)
            continue
        upper = (egs << (steps - 1 - k)) // 2
        group, part = s % 2, s // 2
        bytes_of(rows_of[k], s, k).wait_recv()
        data, scales, total = recv[s][k], srecv[s][k], acc[s]

        near = min(share, 2 * upper if k < steps - 1 else egs)

        def summed(i, data=data, scales=scales, total=total, near=near):
            return total[i] + data[i].astype(jnp.float32) * scales[i // near]

        if k == steps - 1:
            for el in range(egs):
                out_ref[group * egs + el, :, part * LANES : (part + 1) * LANES] = summed(el)
            continue

        far = min(share, upper)

        def forward(g, _, data=data, fresh=sfwd[s][k], summed=summed, upper=upper, far=far):
            qs, scale = quantized([summed(upper + g * far + j) for j in range(far)])
            for j, q in enumerate(qs):
                data[upper + g * far + j] = q
            fresh[g] = scale
            return 0

        def keep(i, _, total=total, summed=summed):
            total[i] = summed(i)
            return 0

        unroll = min(UNROLL, upper)
        lax.fori_loop(0, upper // far, forward, 0, unroll=max(1, unroll // far))
        ship(s, k + 1, data.at[pl.ds(upper, upper)], sfwd[s][k], toward(orders[s][k + 1]))
        lax.fori_loop(0, upper, keep, 0, unroll=unroll)

    x_swap.wait_send()
    remote(dy_hbm, dy_hbm, tok_s.at[1], tok_r.at[0], (mate, me_ex)).wait_send()
    for s in range(streams):
        bytes_of(sum(rows_of), s, 0).wait_send()


def shards(n_dp, n_exp, x_rows, dy_rows, seg_blocks):
    tokens, hid = x_rows.shape
    ffn = dy_rows.shape[1]
    experts = seg_blocks.shape[1]
    egs = experts // 2
    rows_out = hid // n_dp
    fsh = ffn // n_exp
    parts = fsh // LANES
    streams = 2 * parts
    orders, turns = plan(n_dp, n_exp, streams, egs * (hid // 2) * n_exp * LANES * 2)
    steps = len(orders[0])
    sizes = [(1 << (steps - 1 - k)) * egs for k in range(steps)]
    scratch = [
        pltpu.SMEM(seg_blocks.shape[::-1], seg_blocks.dtype),
        pltpu.VMEM(x_rows.shape, x_rows.dtype),
        pltpu.VMEM((2, tokens // BLOCK, hid // 2, BLOCK), x_rows.dtype),
        pltpu.VMEM((tokens // BLOCK, hid // 2, BLOCK), x_rows.dtype),
        pltpu.VMEM((experts, hid // 2, 2 * CAP * BLOCK), x_rows.dtype),
        pltpu.VMEM((n_exp, hid // 2, LANES), jnp.float32),
    ]
    scratch += [pltpu.VMEM((tokens // BLOCK, BLOCK, n_exp * LANES), dy_rows.dtype)] * (2 * parts)
    scratch += [pltpu.VMEM((sizes[0], rows_out, LANES), jnp.float32)] * streams
    scratch += [pltpu.VMEM((sizes[0], rows_out, LANES), jnp.int16)] * streams
    share = SHARE if egs == 1 else 1
    counts = [size // min(share, size) for size in sizes]
    scratch += [pltpu.VMEM((counts[0], 1, LANES), jnp.float32)] * streams
    for _ in range(streams):
        scratch += [pltpu.VMEM((size, rows_out, LANES), jnp.int16) for size in sizes]
    for _ in range(streams):
        scratch += [pltpu.VMEM((count, 1, LANES), jnp.float32) for count in counts]
    for _ in range(streams):
        scratch += [pltpu.VMEM((count, 1, LANES), jnp.float32) for count in counts[1:]]
    scratch += [pltpu.VMEM((sum(sizes) * rows_out // 2 + sum(counts), 1, LANES), jnp.float32)]
    used = sum(math.prod(a.shape) * jnp.dtype(a.dtype).itemsize for a in scratch if a.memory_space == pltpu.VMEM)
    room = min(60 << 20, used + (8 << 20))
    scratch += [pltpu.SemaphoreType.DMA((1 + SLICES + parts,))] + [pltpu.SemaphoreType.DMA((2,)), pltpu.SemaphoreType.DMA((parts + 1,))]
    scratch += [pltpu.SemaphoreType.DMA((streams,)), pltpu.SemaphoreType.DMA((streams, steps))] + [pltpu.SemaphoreType.REGULAR] * 2
    cfg = (n_dp, n_exp, experts, orders, turns, egs, rows_out, parts)
    return pl.pallas_call(
        functools.partial(kernel, cfg),
        out_shape=jax.ShapeDtypeStruct((experts, rows_out, fsh), jnp.float32),
        in_specs=[pl.BlockSpec(memory_space=pl.ANY)] * 3,
        out_specs=pl.BlockSpec(memory_space=pltpu.VMEM),
        scratch_shapes=scratch,
        compiler_params=pltpu.CompilerParams(
            collective_id=0, has_side_effects=True, vmem_limit_bytes=room
        ),
        name="grouped_grad",
    )(*(pltpu.with_memory_space_constraint(a, pltpu.HBM) for a in (seg_blocks.T, x_rows, dy_rows.reshape(-1, BLOCK, ffn))))


def solution(mesh):
    in_specs = (P(("dp", "expert"), None), P(("dp", "expert"), None), P())
    out_specs = P(None, "dp", "expert")
    body = functools.partial(shards, mesh.shape["dp"], mesh.shape["expert"])
    return jax.shard_map(body, mesh=mesh, in_specs=in_specs, out_specs=out_specs, check_vma=False)
```

```python
import functools
import math

import jax
import jax.numpy as jnp
from jax import lax
from jax.experimental import pallas as pl
from jax.experimental.pallas import tpu as pltpu
from jax.sharding import PartitionSpec as P

BLOCK = 128
CAP = 2
LANES = 128
MESH = pl.DeviceIdType.MESH
TOP = 32767.0
UNROLL = 4
FLAT = 16
SLICES = 4
SHARE = 4
AHEAD = 1
LINK = 46.6e3
LATENCY = 2.9
HOP = 0.6
COMPUTE = 0.55
TURN = 0.2
SPEED = 4e5
SWAP = {("dp", 1): ("expert", 0), ("expert", 0): ("dp", 1)}
PATTERN = (
    11, 2, 7, 15, 10, 14, 1, 12, 14, 0, 13, 3, 3, 5, 12, 0,
)
TURNS = (
    0, 1, 2, 3, 4, 5, 6, 7, 2, 8, 0, 9, 5, 4, 1, 10, 11, 12, 13, 7,
    14, 15, 3, 2, 7, 6, 10, 8, 11, 12, 14, 9, 15, 1, 13, 5, 0, 6, 14, 10,
    11, 1, 9, 3, 15, 12, 4, 8, 6, 13, 0, 5, 11, 9, 7, 2, 12, 14, 4, 15,
    13, 10, 3, 1, 8, 14, 5, 12, 11, 2, 7, 10, 0, 15, 4, 3, 9, 6, 13, 8,
)


def bits_of(size):
    count = size.bit_length() - 1
    assert size == 1 << count
    return count


def line_of(way):
    axis, bit = way
    if axis != "dp":
        return axis, 1
    return (axis, 1) if bit == 1 else ("far", 1 << (bit - 2))


def plan(n_dp, n_exp, streams, size):
    dp = [("dp", b) for b in range(1, bits_of(n_dp))]
    ex = [("expert", b) for b in range(bits_of(n_exp))]
    x, z, rest = dp[:1], dp[1:2], dp[2:]
    ways = [
        x + ex + z + rest, ex + x + z + rest, ex + z + x + rest, x + z + ex + rest, z + x + ex + rest, z + ex + x + rest,
        x + z + rest + ex, ex + z + rest + x, z + x + rest + ex, z + ex + rest + x, z + rest + x + ex, z + rest + ex + x,
        x + ex + rest + z, ex + x + rest + z, x + rest + ex + z, ex + rest + x + z,
    ]
    orders = [ways[PATTERN[s % len(PATTERN)]] for s in range(streams)]
    steps = len(orders[0])
    if len(TURNS) == streams * (steps + 1):
        count = [-2] * streams
        turns = []
        for s in TURNS:
            count[s] += 1
            turns.append((s, count[s]))
        return orders, turns
    free, flying, turns, clock, first = {}, [], [], 0.0, 0

    def sent(s, k, now):
        line, hops = line_of(orders[s][k])
        free[line] = max(now, free.get(line, 0.0)) + (size >> (k + 1)) / LINK * hops
        flying.append((free[line] + LATENCY + HOP * (hops - 1), s, k))

    while first < streams or flying:
        landed = [(k, when, s) for when, s, k in flying if when <= clock]
        if not landed and first < streams:
            turns.append((first, -1))
            clock += COMPUTE
            sent(first, 0, clock)
            first += 1
            continue
        if landed:
            k, when, s = min(landed)
        else:
            when, s, k = min(flying)
        flying.remove((when, s, k))
        clock = max(clock, when) + TURN + (size >> (k + 1)) / SPEED
        turns.append((s, k))
        if k + 1 < steps:
            sent(s, k + 1, clock)
    return orders, turns


def quantized(values):
    peak = functools.reduce(jnp.maximum, [jnp.abs(v) for v in values])
    m = jnp.maximum(jnp.max(peak, axis=0, keepdims=True), 1e-30)
    return [jnp.round(v * (TOP / m)).astype(jnp.int32).astype(jnp.int16) for v in values], m * (1.0 / TOP)


def kernel(cfg, counts_hbm, x_hbm, dy_hbm, out_ref, *scratch):
    n_dp, n_exp, experts, orders, turns, egs, rows_out, parts = cfg
    streams = len(orders)
    steps = len(orders[0])
    share = SHARE if egs == 1 else 1
    it = iter(scratch)
    counts_ref, x_ref, x_half, x_got, lhs, temp = (next(it) for _ in range(6))
    dy_own = [next(it) for _ in range(parts)]
    dy_got = [next(it) for _ in range(parts)]
    acc = [next(it) for _ in range(streams)]
    send = [next(it) for _ in range(streams)]
    ssend = [next(it) for _ in range(streams)]
    recv = [[next(it) for _ in range(steps)] for _ in range(streams)]
    srecv = [[next(it) for _ in range(steps)] for _ in range(streams)]
    sfwd = [[next(it) for _ in range(steps - 1)] for _ in range(streams)]
    tally, load, tok_s, tok_r, sent, landed, ready, go = it

    hid = x_ref.shape[1]
    fsh = dy_hbm.shape[2] // n_exp
    blocks = dy_hbm.shape[0]
    me_dp = lax.axis_index("dp")
    me_ex = lax.axis_index("expert")
    core = lax.rem(me_dp, 2)
    mate = me_dp + 1 - 2 * core

    def flip(value, bit):
        own = lax.rem(value // (1 << bit), 2)
        return value + (1 - 2 * own) * (1 << bit)

    def partner(axis, bit):
        return (flip(me_dp, bit), me_ex) if axis == "dp" else (me_dp, flip(me_ex, bit))

    def toward(way):
        dp, ex = partner(*way)
        dp_too, ex_too = partner(*SWAP.get(way, way))
        return dp + core * (dp_too - dp), ex + core * (ex_too - ex)

    wide_x = hid // SLICES
    x_loads = []
    for c in range(SLICES):
        cols = pl.ds(c * wide_x, wide_x)
        x_loads.append(pltpu.make_async_copy(x_hbm.at[:, cols], x_ref.at[:, cols], load.at[1 + c]))
        x_loads[-1].start()
    counts_load = pltpu.make_async_copy(counts_hbm, counts_ref, load.at[0])
    counts_load.start()
    dy_loads = []
    for part in range(parts):
        for y in range(n_exp):
            dy_loads.append(pltpu.make_async_copy(
                dy_hbm.at[:, :, pl.ds(y * fsh + part * LANES, LANES)],
                dy_own[part].at[:, :, pl.ds(y * LANES, LANES)],
                load.at[1 + SLICES + part],
            ))
            dy_loads[-1].start()

    barrier = pltpu.get_barrier_semaphore()
    peers = [partner(*d) for d in orders[0]]

    @pl.when(core == 1)
    def _():
        pl.semaphore_signal(barrier, inc=1, device_id=(mate, me_ex), device_id_type=MESH)

    def remote(src, dst, s_sem, r_sem, peer):
        return pltpu.make_async_remote_copy(
            src_ref=src, dst_ref=dst, send_sem=s_sem, recv_sem=r_sem,
            device_id=peer, device_id_type=MESH,
        )

    per = LANES // (2 * rows_out)

    def turn(j, _):
        xt = x_ref[:, pl.ds(pl.multiple_of(j * LANES, LANES), LANES)].T
        for g in range(per):
            lo = xt[g * 2 * rows_out : g * 2 * rows_out + rows_out]
            hi = xt[g * 2 * rows_out + rows_out : (g + 1) * 2 * rows_out]
            at = pl.ds(pl.multiple_of((j * per + g) * rows_out, rows_out), rows_out)

            for b in range(blocks):
                cut = slice(b * BLOCK, (b + 1) * BLOCK)
                x_half[core, b, at, :] = lo[:, cut]
                x_half[1 - core, b, at, :] = hi[:, cut]
        return 0


    @pl.when(core == 0)
    def _():
        pl.semaphore_wait(barrier, 1)
        pl.semaphore_signal(ready, inc=1, device_id=(mate, me_ex), device_id_type=MESH)

    @pl.when(core == 1)
    def _():
        pl.semaphore_wait(ready, 1)
        for peer in peers:
            pl.semaphore_signal(barrier, inc=1, device_id=peer, device_id_type=MESH)

    mate_copies = []
    for c in range(SLICES):
        x_loads[c].wait()
        lax.fori_loop(c * wide_x // LANES, (c + 1) * wide_x // LANES, turn, 0, unroll=wide_x // LANES)
        at = pl.ds(c * wide_x // 2, wide_x // 2)
        mate_copies.append(remote(x_half.at[1, :, at], x_got.at[:, at], tok_s.at[0], tok_r.at[parts], (mate, me_ex)))
        mate_copies[-1].start()
    for part in range(parts):
        pltpu.make_async_copy(dy_own[part], dy_own[part], load.at[1 + SLICES + part]).wait()
        mate_copies.append(remote(dy_own[part], dy_got[part], tok_s.at[1], tok_r.at[part], (mate, me_ex)))
        if part < AHEAD:
            mate_copies[-1].start()
    counts_load.wait()

    lane = lax.broadcasted_iota(jnp.int32, (1, LANES), 1)

    def segment(dp_index, e):
        row = dp_index * n_exp + me_ex
        start = jnp.int32(0)
        for i in range(experts - 1):
            start = start + jnp.where(i < e, counts_ref[i, row], 0)
        count = counts_ref[e, row]
        return count, [jnp.minimum(start + j, blocks - 1) for j in range(CAP)]

    def packed(ref, dp_index, first):
        def one(e, _):
            count, spots = segment(dp_index, e)
            for j, at in enumerate(spots):
                keep = jnp.where(lane < (count - j) * BLOCK, 1.0, 0.0).astype(jnp.bfloat16)
                lhs[e, :, (first + j) * BLOCK : (first + j + 1) * BLOCK] = ref[at] * keep
            return 0

        lax.fori_loop(0, experts, one, 0)

    packed(x_half.at[0], me_dp, 0)
    x_swap = remote(x_half.at[1], x_got, tok_s.at[0], tok_r.at[parts], (mate, me_ex))
    x_swap.wait_recv()
    packed(x_got, mate, CAP)

    sizes = [ref.shape[0] for ref in recv[0]]
    rows_of = [size * rows_out // 2 + ref.shape[0] for size, ref in zip(sizes, srecv[0])]

    def bytes_of(rows, s, k):
        view = tally.at[pl.ds(0, rows)]
        return remote(view, view, sent.at[s], landed.at[s, k], (mate, me_ex))

    def ship(s, k, src, ssrc, to):
        for pair in (
            remote(ssrc, srecv[s][k], sent.at[s], landed.at[s, k], to),
            remote(src, recv[s][k], sent.at[s], landed.at[s, k], to),
        ):
            pair.start()

    def everyone():
        @pl.when(core == 1)
        def _():
            pl.semaphore_wait(barrier, len(peers))
            pl.semaphore_signal(go, inc=1, device_id=(mate, me_ex), device_id_type=MESH)

        @pl.when(core == 0)
        def _():
            pl.semaphore_wait(go, 1)

    def opening(s):
        order = orders[s]
        group, part = s % 2, s // 2
        half = 1 << (steps - 1)
        goals = [toward(way) for way in order]
        if group == 0:
            if part + AHEAD < parts:
                mate_copies[SLICES + part + AHEAD].start()
            mate_copies[SLICES + part].wait_recv()

        def block_of(place):
            qq, yy = me_dp, me_ex
            for k, (dp, ex) in enumerate(goals):
                r = lax.rem(place // (1 << (steps - 1 - k)), 2)
                qq = qq + r * (dp - me_dp)
                yy = yy + r * (ex - me_ex)
            return temp[yy, pl.ds(pl.multiple_of((qq // 2) * rows_out, rows_out), rows_out), :]

        def per_expert(el, _):
            e = group * egs + el
            spots = [(ref, at) for ref, d in ((dy_own[part], me_dp), (dy_got[part], mate)) for at in segment(d, e)[1]]
            wide = min(2, n_exp)
            for y in range(0, n_exp, wide):
                cols = slice(y * LANES, (y + wide) * LANES)
                rhs = jnp.concatenate([ref[at, :, cols] for ref, at in spots], axis=0)
                got = jnp.dot(lhs[e], rhs, preferred_element_type=jnp.float32)
                for w in range(wide):
                    temp[y + w] = got[:, w * LANES : (w + 1) * LANES]

            near = min(share, half)

            def away(g, _):
                qs, scale = quantized([block_of(half + g * near + j) for j in range(near)])
                for j, q in enumerate(qs):
                    send[s][(g * near + j) * egs + el] = q
                ssend[s][g * egs + el] = scale
                return 0

            def home(p, _):
                acc[s][p * egs + el] = block_of(p)
                return 0

            lax.fori_loop(0, half // near, away, 0, unroll=half // near if half <= FLAT else 1)
            if egs == 1:
                if s == 0:
                    everyone()
                ship(s, 0, send[s], ssend[s], goals[0])
            lax.fori_loop(0, half, home, 0, unroll=half if half <= FLAT else UNROLL)
            return 0

        if egs == 1:
            per_expert(0, 0)
        else:
            lax.fori_loop(0, egs, per_expert, 0)
            if s == 0:
                everyone()
            ship(s, 0, send[s], ssend[s], goals[0])

    for s, k in turns:
        if k < 0:
            opening(s)
            continue
        upper = (egs << (steps - 1 - k)) // 2
        group, part = s % 2, s // 2
        bytes_of(rows_of[k], s, k).wait_recv()
        data, scales, total = recv[s][k], srecv[s][k], acc[s]

        near = min(share, 2 * upper if k < steps - 1 else egs)

        def summed(i, data=data, scales=scales, total=total, near=near):
            return total[i] + data[i].astype(jnp.float32) * scales[i // near]

        if k == steps - 1:
            for el in range(egs):
                out_ref[group * egs + el, :, part * LANES : (part + 1) * LANES] = summed(el)
            continue

        far = min(share, upper)

        def forward(g, _, data=data, fresh=sfwd[s][k], summed=summed, upper=upper, far=far):
            qs, scale = quantized([summed(upper + g * far + j) for j in range(far)])
            for j, q in enumerate(qs):
                data[upper + g * far + j] = q
            fresh[g] = scale
            return 0

        def keep(i, _, total=total, summed=summed):
            total[i] = summed(i)
            return 0

        unroll = min(UNROLL, upper)
        lax.fori_loop(0, upper // far, forward, 0, unroll=max(1, unroll // far))
        ship(s, k + 1, data.at[pl.ds(upper, upper)], sfwd[s][k], toward(orders[s][k + 1]))
        lax.fori_loop(0, upper, keep, 0, unroll=unroll)

    x_swap.wait_send()
    remote(dy_hbm, dy_hbm, tok_s.at[1], tok_r.at[0], (mate, me_ex)).wait_send()
    for s in range(streams):
        bytes_of(sum(rows_of), s, 0).wait_send()


def shards(n_dp, n_exp, x_rows, dy_rows, seg_blocks):
    tokens, hid = x_rows.shape
    ffn = dy_rows.shape[1]
    experts = seg_blocks.shape[1]
    egs = experts // 2
    rows_out = hid // n_dp
    fsh = ffn // n_exp
    parts = fsh // LANES
    streams = 2 * parts
    orders, turns = plan(n_dp, n_exp, streams, egs * (hid // 2) * n_exp * LANES * 2)
    steps = len(orders[0])
    sizes = [(1 << (steps - 1 - k)) * egs for k in range(steps)]
    scratch = [
        pltpu.SMEM(seg_blocks.shape[::-1], seg_blocks.dtype),
        pltpu.VMEM(x_rows.shape, x_rows.dtype),
        pltpu.VMEM((2, tokens // BLOCK, hid // 2, BLOCK), x_rows.dtype),
        pltpu.VMEM((tokens // BLOCK, hid // 2, BLOCK), x_rows.dtype),
        pltpu.VMEM((experts, hid // 2, 2 * CAP * BLOCK), x_rows.dtype),
        pltpu.VMEM((n_exp, hid // 2, LANES), jnp.float32),
    ]
    scratch += [pltpu.VMEM((tokens // BLOCK, BLOCK, n_exp * LANES), dy_rows.dtype)] * (2 * parts)
    scratch += [pltpu.VMEM((sizes[0], rows_out, LANES), jnp.float32)] * streams
    scratch += [pltpu.VMEM((sizes[0], rows_out, LANES), jnp.int16)] * streams
    share = SHARE if egs == 1 else 1
    counts = [size // min(share, size) for size in sizes]
    scratch += [pltpu.VMEM((counts[0], 1, LANES), jnp.float32)] * streams
    for _ in range(streams):
        scratch += [pltpu.VMEM((size, rows_out, LANES), jnp.int16) for size in sizes]
    for _ in range(streams):
        scratch += [pltpu.VMEM((count, 1, LANES), jnp.float32) for count in counts]
    for _ in range(streams):
        scratch += [pltpu.VMEM((count, 1, LANES), jnp.float32) for count in counts[1:]]
    scratch += [pltpu.VMEM((sum(sizes) * rows_out // 2 + sum(counts), 1, LANES), jnp.float32)]
    used = sum(math.prod(a.shape) * jnp.dtype(a.dtype).itemsize for a in scratch if a.memory_space == pltpu.VMEM)
    room = min(60 << 20, used + (8 << 20))
    scratch += [pltpu.SemaphoreType.DMA((1 + SLICES + parts,))] + [pltpu.SemaphoreType.DMA((2,)), pltpu.SemaphoreType.DMA((parts + 1,))]
    scratch += [pltpu.SemaphoreType.DMA((streams,)), pltpu.SemaphoreType.DMA((streams, steps))] + [pltpu.SemaphoreType.REGULAR] * 2
    cfg = (n_dp, n_exp, experts, orders, turns, egs, rows_out, parts)
    return pl.pallas_call(
        functools.partial(kernel, cfg),
        out_shape=jax.ShapeDtypeStruct((experts, rows_out, fsh), jnp.float32),
        in_specs=[pl.BlockSpec(memory_space=pl.ANY)] * 3,
        out_specs=pl.BlockSpec(memory_space=pltpu.VMEM),
        scratch_shapes=scratch,
        compiler_params=pltpu.CompilerParams(
            collective_id=0, has_side_effects=True, vmem_limit_bytes=room
        ),
        name="grouped_grad",
    )(*(pltpu.with_memory_space_constraint(a, pltpu.HBM) for a in (seg_blocks.T, x_rows, dy_rows.reshape(-1, BLOCK, ffn))))


def solution(mesh):
    in_specs = (P(("dp", "expert"), None), P(("dp", "expert"), None), P())
    out_specs = P(None, "dp", "expert")
    body = functools.partial(shards, mesh.shape["dp"], mesh.shape["expert"])
    return jax.shard_map(body, mesh=mesh, in_specs=in_specs, out_specs=out_specs, check_vma=False)
```
